32 devices in a mesh: grp: 8 (over z, x), row: 4 (over y, core).
Axes of the slice: x: 2, y: 2, z: 4, core: 2. Of those that a mesh axis runs over, the one named last changes fastest.
Arguments:
- gll_state: float32 [8, 32, 16, 4096], P(None, None, None, ('grp', 'row')), may hold values from -6 to 6
- metric: float32 [16, 4096], P(None, ('grp', 'row')), may hold values from 0.7 to 1.4
- phys_owner: int32 [4096, 4, 1], P(('grp', 'row')), may hold values from 0 to 7; in each aligned block of 512 rows (0 to 511, 512 to 1023, ..., all dimensions but the last counted through in order) at most 128 rows name the same one
- neighbours: int32 [4, 4096], P(None, ('grp', 'row')), may hold values from 0 to 4095, as said below
- phys_rate: float32 [32, 32768], P(None, ('grp', 'row')), may hold values from 0.2 to 2
- phys_forcing: float32 [32, 32768], P(None, ('grp', 'row')), may hold values from -6 to 6
- field_mix: float32 [8, 8], replicated, may hold values from -2 to 2
Outputs:
- gll_tend: float32 [8, 32, 16, 4096], P(None, None, None, ('grp', 'row'))
The draws below stay inside these ranges and needn't reach their ends.
Inputs may be any that keep to these rules, and one draw needn't show every extreme that they name: `phys_owner`: in the 512 rows of one device, no owner is named more than 128 times, and some owner reaches 128. `neighbours`: rows 0 and 1 of element e are e - 1 and e + 1, cyclically over 4096 elements; rows 2 and 3 lie 2 to 32 positions before and after e, cyclically, and some element has a neighbour exactly 32 positions away.
All inputs are finite; a program needn't handle non-finite values.
Results may differ from the reference program's by a relative error of at most 0.000094.
Values sent between devices are 32-bit elements; how exact they have to be, the bound alone decides.
A program may use at most 64 MiB of HBM per device.

```python
import math
import jax
import jax.numpy as jnp
import numpy as np
from jax import lax

NF = 8
NLEV = 32
NODES = 16
E_DEV = 128
HALO = 32
CAP = 128
ELEMS = 4096
SLOTS = 32768
N_GRP = 8
N_ROW = 4


def draw_neighbours(key, part):
    first_key = jax.random.fold_in(key, 11)
    second_key = jax.random.fold_in(key, 23)
    elem_ids = jnp.arange(ELEMS, dtype=jnp.int32)
    south_step = jax.random.randint(first_key, (ELEMS,), 2, HALO + 1, dtype=jnp.int32)
    north_step = jax.random.randint(second_key, (ELEMS,), 2, HALO + 1, dtype=jnp.int32)
    north_step = jnp.where(elem_ids == 0, HALO, north_step)
    return jnp.stack([(elem_ids - 1) % ELEMS, (elem_ids + 1) % ELEMS, (elem_ids - south_step) % ELEMS, (elem_ids + north_step) % ELEMS]).astype(jnp.int32)


def shard_levels(own_key, dims, shards, smallest, top_value):
    def one(dim, blocks):
        heights = jax.random.uniform(jax.random.fold_in(jax.random.fold_in(own_key, 6), dim), (blocks,), jnp.float32, smallest / len(shards), top_value / len(shards))
        return jnp.repeat(jnp.exp(heights), dims[dim] // blocks).reshape((-1,) + (1,) * (len(dims) - dim - 1))

    gain = one(*shards[0])
    for cut in shards[1:]:
        gain = gain * one(*cut)
    return gain


def routed_block(stream_key, own, number, rows, number_of, top, most, lean):
    sequence = jax.random.permutation(stream_key, number_of)
    crowded, usual = portions_of(number_of, rows * top, most, lean, True), portions_of(number_of, rows * top, most, lean, False)
    places = jnp.arange(number_of)

    def named(tallies, turn):
        used = int((tallies > 0).sum())
        fixed = max(1, used // 4)
        moved = fixed + (places - fixed + turn * (used - fixed)) % max(1, number_of - fixed)
        return jnp.zeros((number_of,), jnp.int32).at[sequence[jnp.where(places < fixed, places, moved)]].set(jnp.asarray(tallies, jnp.int32))

    tallies = jnp.where(number % 4 == 0, named(crowded, number // 4), named(usual, number - number // 4 - 1))
    mixed = jax.random.permutation(jax.random.fold_in(own, 3), number_of)
    donor, sink = mixed[0:number_of // 2 * 2:2], mixed[1:number_of // 2 * 2:2]
    margin = jnp.minimum(tallies[donor] - 1, most - tallies[sink]) // 2
    margin = jnp.where((donor == sequence[0]) | (sink == sequence[0]) | (tallies[sink] == 0), 0, jnp.maximum(margin, 0))
    moved = jax.random.randint(jax.random.fold_in(own, 4), (number_of // 2,), 0, 1 << 20) % (margin + 1)
    tallies = tallies.at[donor].add(-moved).at[sink].add(moved)
    labels = jnp.searchsorted(jnp.cumsum(tallies), jnp.arange(rows * top), side="right").astype(jnp.int32)
    table = labels.reshape(top, rows).T
    table = table[jax.random.permutation(jax.random.fold_in(own, 1), rows)]
    turn = jax.random.randint(jax.random.fold_in(own, 2), (rows, 1), 0, top)
    return jnp.take_along_axis(table, (jnp.arange(top)[None, :] + turn) % top, axis=1)


def portions_of(amount, total, bound, lean, full):
    portions = [(1 << 20) // math.isqrt(grade ** lean) + 1 for grade in range(1, amount + 1)]
    largest = bound if full else min(bound, max(-(-total // amount), total * portions[0] // sum(portions)))
    least = 1 if total - largest >= amount - 1 else 0
    counts, rest = [largest] + [least] * (amount - 1), total - largest - least * (amount - 1)
    while rest > 0:
        free = [i for i in range(1, amount) if counts[i] < largest] or [i for i in range(1, amount) if counts[i] < bound]
        mass, left = sum([portions[i] for i in free]), rest
        for i in free:
            more = min(bound - counts[i], max(1, left * portions[i] // mass), rest)
            counts[i] = counts[i] + more
            rest = rest - more
    return np.array(counts)


def centred(stream_key, extent, width, limit, split=(), kind=jnp.bfloat16):
    loudness = shard_levels(stream_key, extent, split, -0.22, 0.18) if split else 1.0
    values = jax.random.normal(stream_key, extent, jnp.float32) * width * loudness
    return jnp.minimum(jnp.maximum(values, -limit), limit).astype(kind)


def setup_inputs(seed: int = 0) -> dict:
    streams_of = jax.random.split(jax.random.key(seed), 8)
    gll_state = centred(streams_of[0], (NF, NLEV, NODES, ELEMS), 1.0, 6.0, ((3, 32),), jnp.float32)
    metric = jnp.clip(jnp.exp(math.log(1.4) - 0.6931472 * jax.random.uniform(streams_of[1], (NODES, ELEMS), jnp.float32) ** shard_levels(streams_of[1], (NODES, ELEMS), ((1, 32),), -0.2, 0.2)), 0.7, 1.4)
    phys_owner_keys = jax.random.split(jax.random.fold_in(streams_of[2], 1), ELEMS * 4 // (4 * E_DEV))
    phys_owner_turns = jax.random.permutation(jax.random.fold_in(streams_of[2], 3), ELEMS * 4 // (4 * E_DEV))
    phys_owner = jax.vmap(lambda own, number: routed_block(jax.random.fold_in(streams_of[2], 2), own, number, 4 * E_DEV, N_GRP, 1, CAP, 2))(phys_owner_keys, phys_owner_turns).reshape((ELEMS, 4, 1))
    neighbours = draw_neighbours(jax.random.fold_in(streams_of[7], 71), 0)
    phys_rate = jnp.clip(jnp.exp(math.log(2.0) - 2.3025851 * jax.random.uniform(streams_of[4], (NLEV, SLOTS), jnp.float32) ** shard_levels(streams_of[4], (NLEV, SLOTS), ((1, 32),), -0.2, 0.2)), 0.2, 2.0)
    phys_forcing = centred(streams_of[5], (NLEV, SLOTS), 1.0, 6.0, ((1, 32),), jnp.float32)
    field_mix = centred(streams_of[6], (NF, NF), NF ** -0.5, 2.0, (), jnp.float32)
    return dict(gll_state=gll_state, metric=metric, phys_owner=phys_owner, neighbours=neighbours, phys_rate=phys_rate, phys_forcing=phys_forcing, field_mix=field_mix)


def lagrange_value(gll_nodes, node_index, point):
    value = 1.0
    for other_index in range(4):
        if other_index != node_index:
            value = value * (point - gll_nodes[other_index]) / (gll_nodes[node_index] - gll_nodes[other_index])
    return value

def remap_tables():
    gll_nodes = np.array([-1.0, -1.0 / np.sqrt(5.0), 1.0 / np.sqrt(5.0), 1.0])
    offset = 0.5 / np.sqrt(3.0)
    halves = np.zeros((2, 4))
    for node_index in range(4):
        left_sum = lagrange_value(gll_nodes, node_index, -0.5 - offset) + lagrange_value(gll_nodes, node_index, -0.5 + offset)
        right_sum = lagrange_value(gll_nodes, node_index, 0.5 - offset) + lagrange_value(gll_nodes, node_index, 0.5 + offset)
        halves[0, node_index] = 0.5 * left_sum
        halves[1, node_index] = 0.5 * right_sum
    cell_weights = (halves[None, :, None, :] * halves[:, None, :, None]).reshape(4, 16)
    interp_cols = np.stack([0.5 - gll_nodes, 0.5 + gll_nodes], axis=1)
    cell_to_node = (interp_cols[None, :, None, :] * interp_cols[:, None, :, None]).reshape(16, 4)
    node_x = np.tile(gll_nodes, 4)
    node_y = np.repeat(gll_nodes, 4)
    slope_weights = 0.5 * np.stack([np.maximum(0.0, -node_x), np.maximum(0.0, node_x), np.maximum(0.0, -node_y), np.maximum(0.0, node_y)], axis=1)
    return (jnp.asarray(cell_weights, jnp.float32), jnp.asarray(cell_to_node, jnp.float32), jnp.asarray(slope_weights, jnp.float32))

def to_cells(gll_state, metric):
    cell_weights, cell_to_node, slope_weights = remap_tables()
    weighted = cell_weights[:, :, None] * metric[None, :, :]
    cell_area = lax.optimization_barrier(jnp.sum(weighted, axis=1))
    cell_mass = jnp.einsum('cne,flne->flce', weighted, gll_state, precision=lax.Precision.HIGHEST)
    return cell_mass / cell_area[None, None]

def physics(cell_values, relax_rate, forcing, field_mix):
    mixed_fields = jnp.einsum('fg,g...->f...', field_mix, cell_values, precision=lax.Precision.HIGHEST)
    return relax_rate[None] * jnp.tanh(mixed_fields + forcing[None])

def to_nodes(tendency, neighbour_means):
    cell_weights, cell_to_node, slope_weights = remap_tables()
    own_mean = lax.optimization_barrier(jnp.mean(tendency, axis=2))
    reconstructed = jnp.einsum('nc,flce->flne', cell_to_node, tendency, precision=lax.Precision.HIGHEST)
    reconstructed = reconstructed + jnp.einsum('nk,flke->flne', slope_weights, neighbour_means - own_mean[:, :, None], precision=lax.Precision.HIGHEST)
    lower_bound = jnp.minimum(lax.optimization_barrier(jnp.min(tendency, axis=2)), lax.optimization_barrier(jnp.min(neighbour_means, axis=2)))
    upper_bound = jnp.maximum(lax.optimization_barrier(jnp.max(tendency, axis=2)), lax.optimization_barrier(jnp.max(neighbour_means, axis=2)))
    return jnp.clip(reconstructed, lower_bound[:, :, None], upper_bound[:, :, None])

def reference(gll_state, metric, phys_owner, neighbours, phys_rate, phys_forcing, field_mix):
    device_total = N_GRP * N_ROW
    cell_values = to_cells(gll_state, metric)
    owner_grp = phys_owner[:, :, 0].reshape(device_total, 4 * E_DEV)
    onehot = (owner_grp[:, :, None] == jnp.arange(N_GRP, dtype=jnp.int32)[None, None, :]).astype(jnp.int32)
    slot_rank = lax.optimization_barrier(jnp.sum((jnp.cumsum(onehot, axis=1) - onehot) * onehot, axis=2))
    device_index = jnp.arange(device_total, dtype=jnp.int32)[:, None]
    target = ((owner_grp * N_ROW + device_index % N_ROW) * (N_GRP * CAP) + device_index // N_ROW * CAP + slot_rank).astype(jnp.int32)
    target = target.reshape(device_total * E_DEV, 4).T
    relax_rate = phys_rate[:, target]
    forcing = phys_forcing[:, target]
    tendency = physics(cell_values, relax_rate, forcing, field_mix)
    own_mean = lax.optimization_barrier(jnp.mean(tendency, axis=2))
    neighbour_means = own_mean[:, :, neighbours]
    return to_nodes(tendency, neighbour_means)
```

```python
import functools

import jax
import jax.numpy as jnp
import numpy as np
from jax import lax
from jax.experimental import pallas as pl
from jax.experimental.pallas import tpu as pltpu
from jax.sharding import PartitionSpec as P

HALO = 32
MESH = pl.DeviceIdType.MESH
PARTS = 4
LANES = 128
GLL = [-1.0, -1.0 / np.sqrt(5.0), 1.0 / np.sqrt(5.0), 1.0]


def half_weights():
    offset = 0.5 / np.sqrt(3.0)
    halves = np.zeros((2, 4))
    for i in range(4):
        for a, middle in enumerate((-0.5, 0.5)):
            for point in (middle - offset, middle + offset):
                value = 0.5
                for k in range(4):
                    if k != i:
                        value *= (point - GLL[k]) / (GLL[i] - GLL[k])
                halves[a, i] += value
    return halves


def pick(index, values):
    out = jnp.full(index.shape, np.float32(values[-1]), jnp.float32)
    for k in range(len(values) - 1):
        out = jnp.where(index == k, np.float32(values[k]), out)
    return out


def split(x):
    high = x.astype(jnp.bfloat16)
    low = (x - high.astype(jnp.float32)).astype(jnp.bfloat16)
    return high, low


def nodes_writer(row_size, neighbours, fields, elems):
    flat = lax.axis_index("grp") * row_size + lax.axis_index("row")
    inside, places = [], []
    for k in range(4):
        spot = neighbours[k : k + 1] - flat * elems
        within = jnp.where((spot >= 0) & (spot < elems), 1, 0)
        inside.append(jnp.broadcast_to(within, (fields, elems)) == 1)
        places.append(jnp.broadcast_to(neighbours[k : k + 1] % elems, (fields, elems)))
    lane = lax.broadcasted_iota(jnp.int32, (fields, elems), 1)
    sub = lax.broadcasted_iota(jnp.int32, (8, elems), 0)
    gi = pick(sub % 4, GLL)
    gj = [pick(sub // 4, GLL[:2]), pick(sub // 4, GLL[2:])]
    left_x, right_x = 0.5 - gi, 0.5 + gi
    low_y = [0.5 - g for g in gj]
    high_y = [0.5 + g for g in gj]
    slope_left = 0.5 * jnp.maximum(0.0, -gi)
    slope_right = 0.5 * jnp.maximum(0.0, gi)
    slope_y = [0.5 * jnp.maximum(0.0, -gj[0]), 0.5 * jnp.maximum(0.0, gj[1])]

    def take(x, index):
        return jnp.take_along_axis(x, index, axis=1, mode="promise_in_bounds")

    def write(tend_ref, from_left, from_right, p, work_ref, store):
        cells = [tend_ref[pl.ds(c * fields, fields), :] for c in range(4)]
        own = (cells[0] + cells[1] + cells[2] + cells[3]) * np.float32(0.25)
        from_left = pltpu.roll(from_left, (elems - HALO * (p + 1)) % elems, 1)
        if p:
            from_right = pltpu.roll(from_right, elems - HALO * p, 1)
        halo = jnp.where(lane < elems // 2, from_right, from_left)
        around = [
            jnp.where(inside[k], take(own, places[k]), take(halo, places[k])) for k in range(4)
        ]
        low = functools.reduce(jnp.minimum, cells + around)
        high = functools.reduce(jnp.maximum, cells + around)
        for k in range(4):
            work_ref[k] = around[k] - own
        work_ref[4] = low
        work_ref[5] = high
        for f in range(fields):
            cell = [tend_ref[pl.ds(c * fields + f, 1), :] for c in range(4)]
            west, east, south, north, lower, upper = (
                work_ref[k, pl.ds(f, 1), :] for k in range(6)
            )
            bottom = left_x * cell[0] + right_x * cell[1]
            top = left_x * cell[2] + right_x * cell[3]
            slope = slope_left * west + slope_right * east
            for v, side in ((0, south), (1, north)):
                value = low_y[v] * bottom + high_y[v] * top + (slope + slope_y[v] * side)
                store(f, v, jnp.minimum(jnp.maximum(value, lower), upper))

    return write


def exchange_kernel(
    grp_size,
    row_size,
    gll_ref,
    metric_ref,
    owner_ref,
    rate_ref,
    forcing_ref,
    mix_ref,
    neighbours_ref,
    done_ref,
    tail_ref,
    tail_halo_ref,
    gll_v,
    metric_v,
    owner_v,
    mix_v,
    neighbours_v,
    slots_v,
    mixed_v,
    recv_v,
    sel_v,
    tend_v,
    pack_v,
    halo_v,
    work_v,
    gll_sem,
    small_sem,
    slots_sem,
    send_sem,
    recv_sem,
    halo_send_sem,
    halo_recv_sem,
    ready_sem,
    near_sem,
):
    fields, levels, nodes, elems = gll_v.shape
    part = levels // PARTS
    cap = recv_v.shape[3]

    def block_of(peer):
        return pl.ds(pl.multiple_of(peer * cap, cap), cap)

    chunks = gll_sem.shape[0]
    chunk = levels // chunks
    pack = elems // HALO
    packs = part // pack
    me = lax.axis_index("grp")
    row = lax.axis_index("row")
    flat = me * row_size + row
    total = grp_size * row_size
    right = lax.rem(flat + 1, total)
    left = lax.rem(flat + total - 1, total)
    right_id = (right // row_size, lax.rem(right, row_size))
    left_id = (left // row_size, lax.rem(left, row_size))

    barrier = pltpu.get_barrier_semaphore()
    first, last = flat == 0, flat == total - 1

    def greet(when, semaphore, device):
        @pl.when(when)
        def _():
            pl.semaphore_signal(semaphore, inc=1, device_id=device, device_id_type=MESH)

    def hear(when, semaphore):
        @pl.when(when)
        def _():
            pl.semaphore_wait(semaphore, 1)

    for peer in range(1, grp_size):
        greet(peer > me, barrier, (peer, row))
    greet(jnp.logical_not(last), barrier, right_id)
    greet(first, barrier, left_id)

    slot_copies = []
    for h in range(PARTS):
        for kind, ref in enumerate((rate_ref, forcing_ref)):
            copy = pltpu.make_async_copy(
                ref.at[pl.ds(h * part, part)],
                slots_v.at[h, pl.ds(kind * part, part)],
                slots_sem.at[h, kind],
            )
            copy.start()
            slot_copies.append(copy)
    small_copies = []
    for k, (src, dst) in enumerate(
        (
            (owner_ref, owner_v),
            (metric_ref, metric_v),
            (mix_ref, mix_v),
            (neighbours_ref, neighbours_v),
        )
    ):
        copy = pltpu.make_async_copy(src, dst, small_sem.at[k])
        copy.start()
        small_copies.append(copy)
    gll_copies = []
    for k in range(chunks):
        span = pl.ds(k * chunk, chunk)
        copy = pltpu.make_async_copy(gll_ref.at[:, span], gll_v.at[:, span], gll_sem.at[k])
        copy.start()
        gll_copies.append(copy)

    @pl.when(jnp.logical_not(first))
    def _():
        pl.semaphore_wait(barrier, me + jnp.where(last, 2, 1))

    for peer in range(grp_size - 1):
        greet(peer < me, ready_sem.at[me], (peer, row))
    greet(jnp.logical_not(first), near_sem.at[0], left_id)
    greet(last, near_sem.at[1], right_id)

    arrivals = {}
    for h in range(PARTS):
        for i in range(1, grp_size):
            peer = lax.rem(me + i, grp_size)
            arrivals[h, i] = pltpu.make_async_remote_copy(
                src_ref=slots_v.at[h, :, block_of(peer)],
                dst_ref=recv_v.at[h, i - 1],
                send_sem=send_sem,
                recv_sem=recv_sem.at[h],
                device_id=(peer, row),
                device_id_type=MESH,
            )
    for h in range(PARTS):
        for copy in slot_copies[2 * h : 2 * h + 2]:
            copy.wait()
        for i in range(1, grp_size):
            pl.when(me + i >= grp_size)(arrivals[h, i].start)

    def send_later(i):
        @pl.when(me + i < grp_size)
        def _():
            pl.semaphore_wait(ready_sem.at[me + i], 1)
            for h in range(PARTS):
                arrivals[h, i].start()

    for copy in small_copies:
        copy.wait()

    grp_iota = lax.broadcasted_iota(jnp.int32, (grp_size, elems), 0)
    named = [
        jnp.where(owner_v[c] == grp_iota, np.float32(1), np.float32(0)) for c in range(4)
    ]
    before = (
        lax.broadcasted_iota(jnp.int32, (elems, elems), 0)
        < lax.broadcasted_iota(jnp.int32, (elems, elems), 1)
    )
    running = jnp.dot(
        (named[0] + named[1] + named[2] + named[3]).astype(jnp.bfloat16),
        jnp.where(before, np.float32(1), np.float32(0)).astype(jnp.bfloat16),
        preferred_element_type=jnp.float32,
    )
    targets = []
    for c in range(4):
        rank = jnp.sum(named[c] * running, axis=0, keepdims=True).astype(jnp.int32)
        running = running + named[c]
        slot = me - owner_v[c]
        slot = jnp.where(slot < 0, slot + grp_size, slot)
        targets.append(slot * cap + rank)

    blocks = [jnp.broadcast_to(t // LANES, (2 * part, elems)) for t in targets]
    places = [jnp.broadcast_to(t % LANES, (2 * part, elems)) for t in targets]

    halves = half_weights()
    width = fields * nodes
    lane = lax.broadcasted_iota(jnp.int32, (fields, width), 1)
    spread = jnp.where(
        lane // nodes == lax.broadcasted_iota(jnp.int32, (fields, width), 0),
        np.float32(1),
        np.float32(0),
    )
    mix = jnp.dot(
        mix_v[...], spread, precision=lax.Precision.HIGHEST, preferred_element_type=jnp.float32
    )
    node = lane % nodes
    row_node = lax.broadcasted_iota(jnp.int32, (nodes, elems), 0)
    metric = metric_v[...]
    rows, scales = [], []
    for c in range(4):
        a, b = c % 2, c // 2
        rows.append(mix * pick(node % 4, halves[a]) * pick(node // 4, halves[b]))
        weights = pick(row_node % 4, halves[a]) * pick(row_node // 4, halves[b])
        area = jnp.sum(weights * metric, axis=0, keepdims=True)
        scales.append(jnp.broadcast_to(1.0 / area, (fields, elems)))
    scale = jnp.concatenate(scales, axis=0)
    high, low = split(jnp.concatenate(rows, axis=0))
    matrix = jnp.concatenate(
        [
            jnp.concatenate([high, high], axis=1),
            jnp.concatenate([low, jnp.zeros_like(low)], axis=1),
        ],
        axis=0,
    )
    count = 4 * fields

    def weigh(level):
        x = (gll_v[:, level] * metric[None]).reshape(width, elems)
        return jnp.concatenate(split(x), axis=0)

    for k in range(chunks):
        gll_copies[k].wait()

        def remap(j, carry):
            level = k * chunk + 2 * j
            data = jnp.concatenate([weigh(level), weigh(level + 1)], axis=1)
            out = jnp.dot(matrix, data, preferred_element_type=jnp.float32)
            out = out[:count] + out[count:]
            mixed_v[level] = out[:, :elems] * scale
            mixed_v[level + 1] = out[:, elems:] * scale
            return carry

        lax.fori_loop(0, chunk // 2, remap, 0, unroll=True)
        if k + 1 < grp_size:
            send_later(k + 1)

    for i in range(chunks + 1, grp_size):
        send_later(i)

    quarter = lax.broadcasted_iota(jnp.int32, (fields, elems), 1) // HALO
    hear(jnp.logical_not(last), near_sem.at[0])
    hear(first, near_sem.at[1])
    halo_copies = []
    for h in range(PARTS):
        picked = [None] * 4
        whole = recv_v.at[h]
        pltpu.make_async_copy(whole, whole, recv_sem.at[h]).wait()
        for i in range(grp_size):
            if i == 0:
                held = slots_v[h, :, block_of(me)]
            else:
                held = recv_v[h, i - 1]
            for k in range(cap // LANES):
                source = held[:, k * LANES : (k + 1) * LANES]
                for c in range(4):
                    value = jnp.take_along_axis(
                        source, places[c], axis=1, mode="promise_in_bounds"
                    )
                    if picked[c] is None:
                        picked[c] = value
                    else:
                        block = i * (cap // LANES) + k
                        picked[c] = jnp.where(blocks[c] == block, value, picked[c])
        for c in range(4):
            sel_v[h, c] = picked[c]
        for q in range(packs):
            to_right = to_left = None
            for p in range(pack):
                at = q * pack + p
                level = h * part + at
                mean = None
                for c in range(4):
                    span = pl.ds(c * fields, fields)
                    tend = sel_v[h, c, pl.ds(at, 1)] * jnp.tanh(
                        mixed_v[level, span] + sel_v[h, c, pl.ds(part + at, 1)]
                    )
                    if h == PARTS - 1:
                        tail_ref[at, span] = tend
                    else:
                        tend_v[level, span] = tend
                    mean = tend if mean is None else mean + tend
                mean = mean * np.float32(0.25)
                to_r = pltpu.roll(mean, (HALO * (p + 1)) % elems, 1) if (p + 1) % pack else mean
                to_l = pltpu.roll(mean, HALO * p, 1) if p else mean
                to_right = to_r if p == 0 else jnp.where(quarter == p, to_r, to_right)
                to_left = to_l if p == 0 else jnp.where(quarter == p, to_l, to_left)
            pack_v[0, h * packs + q] = to_right
            pack_v[1, h * packs + q] = to_left
        span = pl.ds(h * packs, packs)
        for way, device in ((0, right_id), (1, left_id)):
            copy = pltpu.make_async_remote_copy(
                src_ref=pack_v.at[way, span],
                dst_ref=halo_v.at[way, span],
                send_sem=halo_send_sem.at[h, way],
                recv_sem=halo_recv_sem.at[h, way],
                device_id=device,
                device_id_type=MESH,
            )
            copy.start()
            halo_copies.append(copy)

    pltpu.make_async_copy(recv_v, recv_v, send_sem).wait()
    write = nodes_writer(row_size, neighbours_v[...], fields, elems)
    for h in range(PARTS - 1):
        halo_copies[2 * h].wait()
        halo_copies[2 * h + 1].wait()

        def group(q, carry):
            for p in range(pack):
                level = q * pack + p

                def store(f, v, value):
                    done_ref[f, level, pl.ds(8 * v, 8), :] = value

                write(
                    tend_v.at[level], halo_v[0, q], halo_v[1, q], p, work_v.at[p], store
                )
            return carry

        lax.fori_loop(h * packs, (h + 1) * packs, group, 0)
    for copy in halo_copies[2 * PARTS - 2 :]:
        copy.wait()
    for way in range(2):
        for q in range(packs):
            tail_halo_ref[way, q] = halo_v[way, levels // pack - packs + q]


def last_part_kernel(
    row_size, done_ref, tend_ref, halo_ref, neighbours_ref, out_ref, last_v, work_v, sem
):
    fields, part, nodes, elems = last_v.shape
    pack = elems // HALO
    before = done_ref.shape[1]
    copies = []
    for k in range(before // part):
        span = pl.ds(k * part, part)
        copy = pltpu.make_async_copy(done_ref.at[:, span], out_ref.at[:, span], sem.at[k])
        copy.start()
        copies.append(copy)
    write = nodes_writer(row_size, neighbours_ref[...], fields, elems)
    for q in range(part // pack):
        for p in range(pack):
            level = q * pack + p

            def store(f, v, value):
                last_v[f, level, pl.ds(8 * v, 8), :] = value

            write(
                tend_ref.at[level], halo_ref[0, q], halo_ref[1, q], p, work_v.at[level], store
            )
        copy = pltpu.make_async_copy(
            last_v.at[:, pl.ds(q * pack, pack)],
            out_ref.at[:, pl.ds(before + q * pack, pack)],
            sem.at[before // part + q],
        )
        copy.start()
        copies.append(copy)
    for copy in copies:
        copy.wait()


def on_device(gll_state, metric, phys_owner, neighbours, phys_rate, phys_forcing, field_mix):
    fields, levels, nodes, elems = gll_state.shape
    grp_size = lax.axis_size("grp")
    row_size = lax.axis_size("row")
    capacity = phys_rate.shape[1] // grp_size
    cap = -(-capacity // 128) * 128
    if cap != capacity:
        phys_rate, phys_forcing = (
            jnp.pad(
                x.reshape(levels, grp_size, capacity), ((0, 0), (0, 0), (0, cap - capacity))
            ).reshape(levels, grp_size * cap)
            for x in (phys_rate, phys_forcing)
        )
    owner = phys_owner.transpose(1, 2, 0)
    pack = elems // HALO
    part = levels // PARTS
    chunks = 4
    vmem = pl.BlockSpec(memory_space=pltpu.VMEM)
    hbm = pl.BlockSpec(memory_space=pltpu.HBM)
    before = levels - part
    done, tail, tail_halo = pl.pallas_call(
        functools.partial(exchange_kernel, grp_size, row_size),
        out_shape=(
            jax.ShapeDtypeStruct((fields, before, nodes, elems), jnp.float32),
            jax.ShapeDtypeStruct((part, 4 * fields, elems), jnp.float32),
            jax.ShapeDtypeStruct((2, part // pack, fields, elems), jnp.float32),
        ),
        in_specs=[hbm] * 7,
        out_specs=(vmem, vmem, vmem),
        scratch_shapes=[
            pltpu.VMEM((fields, levels, nodes, elems), jnp.float32),
            pltpu.VMEM((nodes, elems), jnp.float32),
            pltpu.VMEM((4, 1, elems), jnp.int32),
            pltpu.VMEM((fields, fields), jnp.float32),
            pltpu.VMEM((4, elems), jnp.int32),
            pltpu.VMEM((PARTS, 2 * part, grp_size * cap), jnp.float32),
            pltpu.VMEM((levels, 4 * fields, elems), jnp.float32),
            pltpu.VMEM((PARTS, grp_size - 1, 2 * part, cap), jnp.float32),
            pltpu.VMEM((PARTS, 4, 2 * part, elems), jnp.float32),
            pltpu.VMEM((before, 4 * fields, elems), jnp.float32),
            pltpu.VMEM((2, levels // pack, fields, elems), jnp.float32),
            pltpu.VMEM((2, levels // pack, fields, elems), jnp.float32),
            pltpu.VMEM((pack, 6, fields, elems), jnp.float32),
            pltpu.SemaphoreType.DMA((chunks,)),
            pltpu.SemaphoreType.DMA((4,)),
            pltpu.SemaphoreType.DMA((PARTS, 2)),
            pltpu.SemaphoreType.DMA,
            pltpu.SemaphoreType.DMA((PARTS,)),
            pltpu.SemaphoreType.DMA((PARTS, 2)),
            pltpu.SemaphoreType.DMA((PARTS, 2)),
            pltpu.SemaphoreType.REGULAR((grp_size,)),
            pltpu.SemaphoreType.REGULAR((2,)),
        ],
        compiler_params=pltpu.CompilerParams(
            collective_id=0, has_side_effects=True, vmem_limit_bytes=32 * 1024 * 1024
        ),
        name="exchange",
    )(
        *(
            pltpu.with_memory_space_constraint(x, pltpu.HBM)
            for x in (
                gll_state,
                metric,
                owner,
                phys_rate,
                phys_forcing,
                field_mix,
                neighbours,
            )
        )
    )
    anywhere = pl.BlockSpec(memory_space=pl.ANY)
    return pl.pallas_call(
        functools.partial(last_part_kernel, row_size),
        out_shape=jax.ShapeDtypeStruct(gll_state.shape, jnp.float32),
        in_specs=[anywhere, vmem, vmem, vmem],
        out_specs=anywhere,
        scratch_shapes=[
            pltpu.VMEM((fields, part, nodes, elems), jnp.float32),
            pltpu.VMEM((part, 6, fields, elems), jnp.float32),
            pltpu.SemaphoreType.DMA((PARTS - 1 + part // pack,)),
        ],
        compiler_params=pltpu.CompilerParams(vmem_limit_bytes=16 * 1024 * 1024),
        name="last_part",
    )(done, tail, tail_halo, neighbours)


def solution(mesh):
    in_specs = (
        P(None, None, None, ("grp", "row")),
        P(None, ("grp", "row")),
        P(("grp", "row"), None, None),
        P(None, ("grp", "row")),
        P(None, ("grp", "row")),
        P(None, ("grp", "row")),
        P(),
    )
    out_specs = P(None, None, None, ("grp", "row"))
    return jax.shard_map(
        on_device, mesh=mesh, in_specs=in_specs, out_specs=out_specs, check_vma=False
    )
```

```python
import functools

import jax
import jax.numpy as jnp
import numpy as np
from jax import lax
from jax.experimental import pallas as pl
from jax.experimental.pallas import tpu as pltpu
from jax.sharding import PartitionSpec as P

HALO = 32
MESH = pl.DeviceIdType.MESH
PARTS = 4
LANES = 128
GLL = [-1.0, -1.0 / np.sqrt(5.0), 1.0 / np.sqrt(5.0), 1.0]


def half_weights():
    offset = 0.5 / np.sqrt(3.0)
    halves = np.zeros((2, 4))
    for i in range(4):
        for a, middle in enumerate((-0.5, 0.5)):
            for point in (middle - offset, middle + offset):
                value = 0.5
                for k in range(4):
                    if k != i:
                        value *= (point - GLL[k]) / (GLL[i] - GLL[k])
                halves[a, i] += value
    return halves


def pick(index, values):
    out = jnp.full(index.shape, np.float32(values[-1]), jnp.float32)
    for k in range(len(values) - 1):
        out = jnp.where(index == k, np.float32(values[k]), out)
    return out


def split(x):
    high = x.astype(jnp.bfloat16)
    low = (x - high.astype(jnp.float32)).astype(jnp.bfloat16)
    return high, low


def nodes_writer(row_size, neighbours, fields, elems):
    flat = lax.axis_index("grp") * row_size + lax.axis_index("row")
    inside, places = [], []
    for k in range(4):
        spot = neighbours[k : k + 1] - flat * elems
        within = jnp.where((spot >= 0) & (spot < elems), 1, 0)
        inside.append(jnp.broadcast_to(within, (fields, elems)) == 1)
        places.append(jnp.broadcast_to(neighbours[k : k + 1] % elems, (fields, elems)))
    lane = lax.broadcasted_iota(jnp.int32, (fields, elems), 1)
    sub = lax.broadcasted_iota(jnp.int32, (8, elems), 0)
    gi = pick(sub % 4, GLL)
    gj = [pick(sub // 4, GLL[:2]), pick(sub // 4, GLL[2:])]
    left_x, right_x = 0.5 - gi, 0.5 + gi
    low_y = [0.5 - g for g in gj]
    high_y = [0.5 + g for g in gj]
    slope_left = 0.5 * jnp.maximum(0.0, -gi)
    slope_right = 0.5 * jnp.maximum(0.0, gi)
    slope_y = [0.5 * jnp.maximum(0.0, -gj[0]), 0.5 * jnp.maximum(0.0, gj[1])]

    def take(x, index):
        return jnp.take_along_axis(x, index, axis=1, mode="promise_in_bounds")

    def write(tend_ref, from_left, from_right, p, work_ref, store):
        cells = [tend_ref[pl.ds(c * fields, fields), :] for c in range(4)]
        own = (cells[0] + cells[1] + cells[2] + cells[3]) * np.float32(0.25)
        from_left = pltpu.roll(from_left, (elems - HALO * (p + 1)) % elems, 1)
        if p:
            from_right = pltpu.roll(from_right, elems - HALO * p, 1)
        halo = jnp.where(lane < elems // 2, from_right, from_left)
        around = [
            jnp.where(inside[k], take(own, places[k]), take(halo, places[k])) for k in range(4)
        ]
        low = functools.reduce(jnp.minimum, cells + around)
        high = functools.reduce(jnp.maximum, cells + around)
        for k in range(4):
            work_ref[k] = around[k] - own
        work_ref[4] = low
        work_ref[5] = high
        for f in range(fields):
            cell = [tend_ref[pl.ds(c * fields + f, 1), :] for c in range(4)]
            west, east, south, north, lower, upper = (
                work_ref[k, pl.ds(f, 1), :] for k in range(6)
            )
            bottom = left_x * cell[0] + right_x * cell[1]
            top = left_x * cell[2] + right_x * cell[3]
            slope = slope_left * west + slope_right * east
            for v, side in ((0, south), (1, north)):
                value = low_y[v] * bottom + high_y[v] * top + (slope + slope_y[v] * side)
                store(f, v, jnp.minimum(jnp.maximum(value, lower), upper))

    return write


def exchange_kernel(
    grp_size,
    row_size,
    gll_ref,
    metric_ref,
    owner_ref,
    rate_ref,
    forcing_ref,
    mix_ref,
    neighbours_ref,
    done_ref,
    tail_ref,
    tail_halo_ref,
    gll_v,
    metric_v,
    owner_v,
    mix_v,
    neighbours_v,
    slots_v,
    mixed_v,
    recv_v,
    sel_v,
    tend_v,
    pack_v,
    halo_v,
    work_v,
    gll_sem,
    small_sem,
    slots_sem,
    send_sem,
    recv_sem,
    halo_send_sem,
    halo_recv_sem,
    ready_sem,
    near_sem,
):
    fields, levels, nodes, elems = gll_v.shape
    part = levels // PARTS
    cap = recv_v.shape[3]

    def block_of(peer):
        return pl.ds(pl.multiple_of(peer * cap, cap), cap)

    chunks = gll_sem.shape[0]
    chunk = levels // chunks
    pack = elems // HALO
    packs = part // pack
    me = lax.axis_index("grp")
    row = lax.axis_index("row")
    flat = me * row_size + row
    total = grp_size * row_size
    right = lax.rem(flat + 1, total)
    left = lax.rem(flat + total - 1, total)
    right_id = (right // row_size, lax.rem(right, row_size))
    left_id = (left // row_size, lax.rem(left, row_size))

    barrier = pltpu.get_barrier_semaphore()
    first, last = flat == 0, flat == total - 1

    def greet(when, semaphore, device):
        @pl.when(when)
        def _():
            pl.semaphore_signal(semaphore, inc=1, device_id=device, device_id_type=MESH)

    def hear(when, semaphore):
        @pl.when(when)
        def _():
            pl.semaphore_wait(semaphore, 1)

    for peer in range(1, grp_size):
        greet(peer > me, barrier, (peer, row))
    for peer in range(1, row_size):
        greet(peer > row, barrier, (me, peer))
    greet(first, barrier, left_id)

    slot_copies = []
    for h in range(PARTS):
        for kind, ref in enumerate((rate_ref, forcing_ref)):
            copy = pltpu.make_async_copy(
                ref.at[pl.ds(h * part, part)],
                slots_v.at[h, pl.ds(kind * part, part)],
                slots_sem.at[h, kind],
            )
            copy.start()
            slot_copies.append(copy)
    small_copies = []
    for k, (src, dst) in enumerate(
        (
            (owner_ref, owner_v),
            (metric_ref, metric_v),
            (mix_ref, mix_v),
            (neighbours_ref, neighbours_v),
        )
    ):
        copy = pltpu.make_async_copy(src, dst, small_sem.at[k])
        copy.start()
        small_copies.append(copy)
    gll_copies = []
    for k in range(chunks):
        span = pl.ds(k * chunk, chunk)
        copy = pltpu.make_async_copy(gll_ref.at[:, span], gll_v.at[:, span], gll_sem.at[k])
        copy.start()
        gll_copies.append(copy)

    @pl.when(jnp.logical_not(first))
    def _():
        pl.semaphore_wait(barrier, me + row + jnp.where(last, 1, 0))

    for peer in range(grp_size - 1):
        greet(peer < me, ready_sem.at[me], (peer, row))
    greet(row > 0, near_sem.at[0], left_id)
    greet(last, near_sem.at[1], right_id)

    arrivals = {}
    for h in range(PARTS):
        for i in range(1, grp_size):
            peer = lax.rem(me + i, grp_size)
            arrivals[h, i] = pltpu.make_async_remote_copy(
                src_ref=slots_v.at[h, :, block_of(peer)],
                dst_ref=recv_v.at[h, i - 1],
                send_sem=send_sem,
                recv_sem=recv_sem.at[h],
                device_id=(peer, row),
                device_id_type=MESH,
            )
    for copy in slot_copies:
        copy.wait()
    for g in range(2):
        for h in range(PARTS):
            for i in range(1, grp_size):
                j = me + i - grp_size
                ok = jnp.logical_and(j >= 0, (j < grp_size // 4) == (g == 0))
                pl.when(ok)(arrivals[h, i].start)

    def send_later(i):
        @pl.when(me + i < grp_size)
        def _():
            pl.semaphore_wait(ready_sem.at[me + i], 1)

        if i == 1:
            greet(
                jnp.logical_and(me < grp_size - 1, row == row_size - 1),
                near_sem.at[1],
                right_id,
            )

        @pl.when(me + i < grp_size - 1)
        def _():
            for h in range(PARTS // 2):
                arrivals[h, i].start()

        @pl.when(me + i == grp_size - 1)
        def _():
            for h in range(PARTS):
                arrivals[h, i].start()

    def send_rest():
        for h in range(PARTS // 2, PARTS):
            for i in range(1, grp_size):
                pl.when(me + i < grp_size - 1)(arrivals[h, i].start)

    for copy in small_copies:
        copy.wait()

    grp_iota = lax.broadcasted_iota(jnp.int32, (grp_size, elems), 0)
    named = [
        jnp.where(owner_v[c] == grp_iota, np.float32(1), np.float32(0)) for c in range(4)
    ]
    before = (
        lax.broadcasted_iota(jnp.int32, (elems, elems), 0)
        < lax.broadcasted_iota(jnp.int32, (elems, elems), 1)
    )
    running = jnp.dot(
        (named[0] + named[1] + named[2] + named[3]).astype(jnp.bfloat16),
        jnp.where(before, np.float32(1), np.float32(0)).astype(jnp.bfloat16),
        preferred_element_type=jnp.float32,
    )
    targets = []
    for c in range(4):
        rank = jnp.sum(named[c] * running, axis=0, keepdims=True).astype(jnp.int32)
        running = running + named[c]
        slot = me - owner_v[c]
        slot = jnp.where(slot < 0, slot + grp_size, slot)
        targets.append(slot * cap + rank)

    blocks = [jnp.broadcast_to(t // LANES, (2 * part, elems)) for t in targets]
    places = [jnp.broadcast_to(t % LANES, (2 * part, elems)) for t in targets]

    halves = half_weights()
    width = fields * nodes
    lane = lax.broadcasted_iota(jnp.int32, (fields, width), 1)
    spread = jnp.where(
        lane // nodes == lax.broadcasted_iota(jnp.int32, (fields, width), 0),
        np.float32(1),
        np.float32(0),
    )
    mix = jnp.dot(
        mix_v[...], spread, precision=lax.Precision.HIGHEST, preferred_element_type=jnp.float32
    )
    node = lane % nodes
    row_node = lax.broadcasted_iota(jnp.int32, (nodes, elems), 0)
    metric = metric_v[...]
    rows, scales = [], []
    for c in range(4):
        a, b = c % 2, c // 2
        rows.append(mix * pick(node % 4, halves[a]) * pick(node // 4, halves[b]))
        weights = pick(row_node % 4, halves[a]) * pick(row_node // 4, halves[b])
        area = jnp.sum(weights * metric, axis=0, keepdims=True)
        scales.append(jnp.broadcast_to(1.0 / area, (fields, elems)))
    scale = jnp.concatenate(scales, axis=0)
    high, low = split(jnp.concatenate(rows, axis=0))
    matrix = jnp.concatenate(
        [
            jnp.concatenate([high, high], axis=1),
            jnp.concatenate([low, jnp.zeros_like(low)], axis=1),
        ],
        axis=0,
    )
    count = 4 * fields

    def weigh(level):
        x = (gll_v[:, level] * metric[None]).reshape(width, elems)
        return jnp.concatenate(split(x), axis=0)

    for k in range(chunks):
        gll_copies[k].wait()

        def remap(j, carry):
            level = k * chunk + 2 * j
            data = jnp.concatenate([weigh(level), weigh(level + 1)], axis=1)
            out = jnp.dot(matrix, data, preferred_element_type=jnp.float32)
            out = out[:count] + out[count:]
            mixed_v[level] = out[:, :elems] * scale
            mixed_v[level + 1] = out[:, elems:] * scale
            return carry

        lax.fori_loop(0, chunk // 2, remap, 0, unroll=True)
        if k + 1 < grp_size:
            send_later(k + 1)

    for i in range(chunks + 1, grp_size):
        send_later(i)
    send_rest()

    quarter = lax.broadcasted_iota(jnp.int32, (fields, elems), 1) // HALO
    hear(row < row_size - 1, near_sem.at[0])
    hear(row == 0, near_sem.at[1])
    halo_copies = []
    for h in range(PARTS):
        picked = [None] * 4
        whole = recv_v.at[h]
        pltpu.make_async_copy(whole, whole, recv_sem.at[h]).wait()
        for i in range(grp_size):
            if i == 0:
                held = slots_v[h, :, block_of(me)]
            else:
                held = recv_v[h, i - 1]
            for k in range(cap // LANES):
                source = held[:, k * LANES : (k + 1) * LANES]
                for c in range(4):
                    value = jnp.take_along_axis(
                        source, places[c], axis=1, mode="promise_in_bounds"
                    )
                    if picked[c] is None:
                        picked[c] = value
                    else:
                        block = i * (cap // LANES) + k
                        picked[c] = jnp.where(blocks[c] == block, value, picked[c])
        for c in range(4):
            sel_v[h, c] = picked[c]
        for q in range(packs):
            to_right = to_left = None
            for p in range(pack):
                at = q * pack + p
                level = h * part + at
                mean = None
                for c in range(4):
                    span = pl.ds(c * fields, fields)
                    tend = sel_v[h, c, pl.ds(at, 1)] * jnp.tanh(
                        mixed_v[level, span] + sel_v[h, c, pl.ds(part + at, 1)]
                    )
                    if h == PARTS - 1:
                        tail_ref[at, span] = tend
                    else:
                        tend_v[level, span] = tend
                    mean = tend if mean is None else mean + tend
                mean = mean * np.float32(0.25)
                to_r = pltpu.roll(mean, (HALO * (p + 1)) % elems, 1) if (p + 1) % pack else mean
                to_l = pltpu.roll(mean, HALO * p, 1) if p else mean
                to_right = to_r if p == 0 else jnp.where(quarter == p, to_r, to_right)
                to_left = to_l if p == 0 else jnp.where(quarter == p, to_l, to_left)
            pack_v[0, h * packs + q] = to_right
            pack_v[1, h * packs + q] = to_left
        span = pl.ds(h * packs, packs)
        for way, device in ((0, right_id), (1, left_id)):
            copy = pltpu.make_async_remote_copy(
                src_ref=pack_v.at[way, span],
                dst_ref=halo_v.at[way, span],
                send_sem=halo_send_sem.at[h, way],
                recv_sem=halo_recv_sem.at[h, way],
                device_id=device,
                device_id_type=MESH,
            )
            copy.start()
            halo_copies.append(copy)

    pltpu.make_async_copy(recv_v, recv_v, send_sem).wait()
    write = nodes_writer(row_size, neighbours_v[...], fields, elems)
    for h in range(PARTS - 1):
        halo_copies[2 * h].wait()
        halo_copies[2 * h + 1].wait()

        def group(q, carry):
            for p in range(pack):
                level = q * pack + p

                def store(f, v, value):
                    done_ref[f, level, pl.ds(8 * v, 8), :] = value

                write(
                    tend_v.at[level], halo_v[0, q], halo_v[1, q], p, work_v.at[p], store
                )
            return carry

        lax.fori_loop(h * packs, (h + 1) * packs, group, 0)
    for copy in halo_copies[2 * PARTS - 2 :]:
        copy.wait()
    for way in range(2):
        for q in range(packs):
            tail_halo_ref[way, q] = halo_v[way, levels // pack - packs + q]


def last_part_kernel(
    row_size, done_ref, tend_ref, halo_ref, neighbours_ref, out_ref, last_v, work_v, sem
):
    fields, part, nodes, elems = last_v.shape
    pack = elems // HALO
    before = done_ref.shape[1]
    copies = []
    for k in range(before // part):
        span = pl.ds(k * part, part)
        copy = pltpu.make_async_copy(done_ref.at[:, span], out_ref.at[:, span], sem.at[k])
        copy.start()
        copies.append(copy)
    write = nodes_writer(row_size, neighbours_ref[...], fields, elems)
    for q in range(part // pack):
        for p in range(pack):
            level = q * pack + p

            def store(f, v, value):
                last_v[f, level, pl.ds(8 * v, 8), :] = value

            write(
                tend_ref.at[level], halo_ref[0, q], halo_ref[1, q], p, work_v.at[level], store
            )
        copy = pltpu.make_async_copy(
            last_v.at[:, pl.ds(q * pack, pack)],
            out_ref.at[:, pl.ds(before + q * pack, pack)],
            sem.at[before // part + q],
        )
        copy.start()
        copies.append(copy)
    for copy in copies:
        copy.wait()


def on_device(gll_state, metric, phys_owner, neighbours, phys_rate, phys_forcing, field_mix):
    fields, levels, nodes, elems = gll_state.shape
    grp_size = lax.axis_size("grp")
    row_size = lax.axis_size("row")
    capacity = phys_rate.shape[1] // grp_size
    cap = -(-capacity // 128) * 128
    if cap != capacity:
        phys_rate, phys_forcing = (
            jnp.pad(
                x.reshape(levels, grp_size, capacity), ((0, 0), (0, 0), (0, cap - capacity))
            ).reshape(levels, grp_size * cap)
            for x in (phys_rate, phys_forcing)
        )
    owner = phys_owner.transpose(1, 2, 0)
    pack = elems // HALO
    part = levels // PARTS
    chunks = 4
    vmem = pl.BlockSpec(memory_space=pltpu.VMEM)
    hbm = pl.BlockSpec(memory_space=pltpu.HBM)
    before = levels - part
    done, tail, tail_halo = pl.pallas_call(
        functools.partial(exchange_kernel, grp_size, row_size),
        out_shape=(
            jax.ShapeDtypeStruct((fields, before, nodes, elems), jnp.float32),
            jax.ShapeDtypeStruct((part, 4 * fields, elems), jnp.float32),
            jax.ShapeDtypeStruct((2, part // pack, fields, elems), jnp.float32),
        ),
        in_specs=[hbm] * 7,
        out_specs=(vmem, vmem, vmem),
        scratch_shapes=[
            pltpu.VMEM((fields, levels, nodes, elems), jnp.float32),
            pltpu.VMEM((nodes, elems), jnp.float32),
            pltpu.VMEM((4, 1, elems), jnp.int32),
            pltpu.VMEM((fields, fields), jnp.float32),
            pltpu.VMEM((4, elems), jnp.int32),
            pltpu.VMEM((PARTS, 2 * part, grp_size * cap), jnp.float32),
            pltpu.VMEM((levels, 4 * fields, elems), jnp.float32),
            pltpu.VMEM((PARTS, grp_size - 1, 2 * part, cap), jnp.float32),
            pltpu.VMEM((PARTS, 4, 2 * part, elems), jnp.float32),
            pltpu.VMEM((before, 4 * fields, elems), jnp.float32),
            pltpu.VMEM((2, levels // pack, fields, elems), jnp.float32),
            pltpu.VMEM((2, levels // pack, fields, elems), jnp.float32),
            pltpu.VMEM((pack, 6, fields, elems), jnp.float32),
            pltpu.SemaphoreType.DMA((chunks,)),
            pltpu.SemaphoreType.DMA((4,)),
            pltpu.SemaphoreType.DMA((PARTS, 2)),
            pltpu.SemaphoreType.DMA,
            pltpu.SemaphoreType.DMA((PARTS,)),
            pltpu.SemaphoreType.DMA((PARTS, 2)),
            pltpu.SemaphoreType.DMA((PARTS, 2)),
            pltpu.SemaphoreType.REGULAR((grp_size,)),
            pltpu.SemaphoreType.REGULAR((2,)),
        ],
        compiler_params=pltpu.CompilerParams(
            collective_id=0, has_side_effects=True, vmem_limit_bytes=32 * 1024 * 1024
        ),
        name="exchange",
    )(
        *(
            pltpu.with_memory_space_constraint(x, pltpu.HBM)
            for x in (
                gll_state,
                metric,
                owner,
                phys_rate,
                phys_forcing,
                field_mix,
                neighbours,
            )
        )
    )
    anywhere = pl.BlockSpec(memory_space=pl.ANY)
    return pl.pallas_call(
        functools.partial(last_part_kernel, row_size),
        out_shape=jax.ShapeDtypeStruct(gll_state.shape, jnp.float32),
        in_specs=[anywhere, vmem, vmem, vmem],
        out_specs=anywhere,
        scratch_shapes=[
            pltpu.VMEM((fields, part, nodes, elems), jnp.float32),
            pltpu.VMEM((part, 6, fields, elems), jnp.float32),
            pltpu.SemaphoreType.DMA((PARTS - 1 + part // pack,)),
        ],
        compiler_params=pltpu.CompilerParams(vmem_limit_bytes=16 * 1024 * 1024),
        name="last_part",
    )(done, tail, tail_halo, neighbours)


def solution(mesh):
    in_specs = (
        P(None, None, None, ("grp", "row")),
        P(None, ("grp", "row")),
        P(("grp", "row"), None, None),
        P(None, ("grp", "row")),
        P(None, ("grp", "row")),
        P(None, ("grp", "row")),
        P(),
    )
    out_specs = P(None, None, None, ("grp", "row"))
    return jax.shard_map(
        on_device, mesh=mesh, in_specs=in_specs, out_specs=out_specs, check_vma=False
    )
```

```python
import functools

import jax
import jax.numpy as jnp
import numpy as np
from jax import lax
from jax.experimental import pallas as pl
from jax.experimental.pallas import tpu as pltpu
from jax.sharding import PartitionSpec as P

HALO = 32
MESH = pl.DeviceIdType.MESH
PARTS = 4
LANES = 128
GLL = [-1.0, -1.0 / np.sqrt(5.0), 1.0 / np.sqrt(5.0), 1.0]


def half_weights():
    offset = 0.5 / np.sqrt(3.0)
    halves = np.zeros((2, 4))
    for i in range(4):
        for a, middle in enumerate((-0.5, 0.5)):
            for point in (middle - offset, middle + offset):
                value = 0.5
                for k in range(4):
                    if k != i:
                        value *= (point - GLL[k]) / (GLL[i] - GLL[k])
                halves[a, i] += value
    return halves


def pick(index, values):
    out = jnp.full(index.shape, np.float32(values[-1]), jnp.float32)
    for k in range(len(values) - 1):
        out = jnp.where(index == k, np.float32(values[k]), out)
    return out


def split(x):
    high = x.astype(jnp.bfloat16)
    low = (x - high.astype(jnp.float32)).astype(jnp.bfloat16)
    return high, low


def nodes_writer(row_size, neighbours, fields, elems):
    flat = lax.axis_index("grp") * row_size + lax.axis_index("row")
    inside, places = [], []
    for k in range(4):
        spot = neighbours[k : k + 1] - flat * elems
        within = jnp.where((spot >= 0) & (spot < elems), 1, 0)
        inside.append(jnp.broadcast_to(within, (fields, elems)) == 1)
        places.append(jnp.broadcast_to(neighbours[k : k + 1] % elems, (fields, elems)))
    lane = lax.broadcasted_iota(jnp.int32, (fields, elems), 1)
    sub = lax.broadcasted_iota(jnp.int32, (8, elems), 0)
    gi = pick(sub % 4, GLL)
    gj = [pick(sub // 4, GLL[:2]), pick(sub // 4, GLL[2:])]
    left_x, right_x = 0.5 - gi, 0.5 + gi
    low_y = [0.5 - g for g in gj]
    high_y = [0.5 + g for g in gj]
    slope_left = 0.5 * jnp.maximum(0.0, -gi)
    slope_right = 0.5 * jnp.maximum(0.0, gi)
    slope_y = [0.5 * jnp.maximum(0.0, -gj[0]), 0.5 * jnp.maximum(0.0, gj[1])]

    def take(x, index):
        return jnp.take_along_axis(x, index, axis=1, mode="promise_in_bounds")

    def write(tend_ref, from_left, from_right, p, work_ref, store):
        cells = [tend_ref[pl.ds(c * fields, fields), :] for c in range(4)]
        own = (cells[0] + cells[1] + cells[2] + cells[3]) * np.float32(0.25)
        from_left = pltpu.roll(from_left, (elems - HALO * (p + 1)) % elems, 1)
        if p:
            from_right = pltpu.roll(from_right, elems - HALO * p, 1)
        halo = jnp.where(lane < elems // 2, from_right, from_left)
        around = [
            jnp.where(inside[k], take(own, places[k]), take(halo, places[k])) for k in range(4)
        ]
        low = functools.reduce(jnp.minimum, cells + around)
        high = functools.reduce(jnp.maximum, cells + around)
        for k in range(4):
            work_ref[k] = around[k] - own
        work_ref[4] = low
        work_ref[5] = high
        for f in range(fields):
            cell = [tend_ref[pl.ds(c * fields + f, 1), :] for c in range(4)]
            west, east, south, north, lower, upper = (
                work_ref[k, pl.ds(f, 1), :] for k in range(6)
            )
            bottom = left_x * cell[0] + right_x * cell[1]
            top = left_x * cell[2] + right_x * cell[3]
            slope = slope_left * west + slope_right * east
            for v, side in ((0, south), (1, north)):
                value = low_y[v] * bottom + high_y[v] * top + (slope + slope_y[v] * side)
                store(f, v, jnp.minimum(jnp.maximum(value, lower), upper))

    return write


def exchange_kernel(
    grp_size,
    row_size,
    gll_ref,
    metric_ref,
    owner_ref,
    rate_ref,
    forcing_ref,
    mix_ref,
    neighbours_ref,
    done_ref,
    tail_ref,
    tail_halo_ref,
    gll_v,
    metric_v,
    owner_v,
    mix_v,
    neighbours_v,
    slots_v,
    mixed_v,
    recv_v,
    sel_v,
    tend_v,
    pack_v,
    halo_v,
    work_v,
    gll_sem,
    small_sem,
    slots_sem,
    send_sem,
    recv_sem,
    halo_send_sem,
    halo_recv_sem,
    ready_sem,
    near_sem,
    far_sem,
):
    fields, levels, nodes, elems = gll_v.shape
    part = levels // PARTS
    cap = recv_v.shape[3]

    def block_of(peer):
        return pl.ds(pl.multiple_of(peer * cap, cap), cap)

    chunks = gll_sem.shape[0]
    chunk = levels // chunks
    pack = elems // HALO
    packs = part // pack
    me = lax.axis_index("grp")
    row = lax.axis_index("row")
    flat = me * row_size + row
    total = grp_size * row_size
    right = lax.rem(flat + 1, total)
    left = lax.rem(flat + total - 1, total)
    right_id = (right // row_size, lax.rem(right, row_size))
    left_id = (left // row_size, lax.rem(left, row_size))

    barrier = pltpu.get_barrier_semaphore()
    first, last = flat == 0, flat == total - 1

    def greet(when, semaphore, device):
        @pl.when(when)
        def _():
            pl.semaphore_signal(semaphore, inc=1, device_id=device, device_id_type=MESH)

    def hear(when, semaphore):
        @pl.when(when)
        def _():
            pl.semaphore_wait(semaphore, 1)

    wide = 2 if grp_size % 2 == 0 else 1
    deep, side = me // wide, lax.rem(me, wide)
    even = lax.rem(row, 2) == 0
    slot_copies = []
    for h in range(PARTS):
        for kind, ref in enumerate((rate_ref, forcing_ref)):
            copy = pltpu.make_async_copy(
                ref.at[pl.ds(h * part, part)],
                slots_v.at[h, pl.ds(kind * part, part)],
                slots_sem.at[h, kind],
            )
            copy.start()
            slot_copies.append(copy)
    for peer in range(1, grp_size):
        greet(
            jnp.logical_and(peer > me, side <= peer % wide), barrier, (peer, row)
        )
    odd = jnp.logical_not(even)
    greet(odd, barrier, (me, row - 1))
    greet(jnp.logical_and(odd, row < row_size - 1), barrier, (me, row + 1))
    greet(row == 1, barrier, (me, row_size - 1))

    small_copies = []
    for k, (src, dst) in enumerate(
        (
            (owner_ref, owner_v),
            (metric_ref, metric_v),
            (mix_ref, mix_v),
            (neighbours_ref, neighbours_v),
        )
    ):
        copy = pltpu.make_async_copy(src, dst, small_sem.at[k])
        copy.start()
        small_copies.append(copy)
    gll_copies = []
    for k in range(chunks):
        span = pl.ds(k * chunk, chunk)
        copy = pltpu.make_async_copy(gll_ref.at[:, span], gll_v.at[:, span], gll_sem.at[k])
        copy.start()
        gll_copies.append(copy)

    def count(*conditions):
        return sum(jnp.where(c, 1, 0) for c in conditions)

    heard = (
        (deep + 1) * (side + 1)
        - 1
        + count(even, jnp.logical_and(even, row > 0), row == row_size - 1)
    )

    @pl.when(heard > 0)
    def _():
        pl.semaphore_wait(barrier, heard)

    for peer in range(grp_size - 1):
        greet(
            jnp.logical_and(peer < me, peer % wide <= side), ready_sem.at[me], (peer, row)
        )
    greet(jnp.logical_and(even, row > 0), near_sem.at[0], (me, row - 1))
    greet(even, near_sem.at[1], (me, row + 1))
    greet(row == row_size - 1, far_sem.at[0], (me, 1))

    arrivals = {}
    for h in range(PARTS):
        for i in range(1, grp_size):
            peer = lax.rem(me + i, grp_size)
            arrivals[h, i] = pltpu.make_async_remote_copy(
                src_ref=slots_v.at[h, :, block_of(peer)],
                dst_ref=recv_v.at[h, i - 1],
                send_sem=send_sem,
                recv_sem=recv_sem.at[h],
                device_id=(peer, row),
                device_id_type=MESH,
            )
    for copy in slot_copies:
        copy.wait()

    def send_to(j, parts, when):
        @pl.when(jnp.logical_and(j < me, when))
        def _():
            i = j + grp_size - me
            for h in parts:
                pltpu.make_async_remote_copy(
                    src_ref=slots_v.at[h, :, pl.ds(j * cap, cap)],
                    dst_ref=recv_v.at[h, i - 1],
                    send_sem=send_sem,
                    recv_sem=recv_sem.at[h],
                    device_id=(j, row),
                    device_id_type=MESH,
                ).start()

    def send_back(allowed, parts, when):
        for j in range(grp_size // 4):
            if allowed(j):
                send_to(j, parts, when(j))
        for some in (parts[: len(parts) // 2], parts[len(parts) // 2 :]):
            for j in range(grp_size // 4, grp_size - 1):
                if some and allowed(j):
                    send_to(j, some, when(j))

    every = list(range(PARTS))
    send_back(lambda j: True, every, lambda j: side >= j % wide)

    def send_one(i, when):
        @pl.when(
            jnp.logical_and(
                jnp.logical_and(when, me + i < grp_size - 1), row < row_size - 1
            )
        )
        def _():
            for h in range(PARTS // 2):
                arrivals[h, i].start()

        @pl.when(jnp.logical_and(when, me + i == grp_size - 1))
        def _():
            for h in range(PARTS):
                arrivals[h, i].start()

    def send_later(i):
        above = jnp.logical_and(me + i < grp_size, lax.rem(me + i, wide) >= side)

        @pl.when(above)
        def _():
            pl.semaphore_wait(ready_sem.at[me + i], 1)

        if wide == 2 and i % 2 == 0:
            send_one(i - 1, jnp.logical_and(above, side == 1))
        send_one(i, above)
        if i == 1:
            if wide == 2:
                send_back(lambda j: j % wide == 1, every, lambda j: side == 0)

            @pl.when(row == 1)
            def _():
                pl.semaphore_wait(near_sem.at[1], 1)
                pl.semaphore_wait(far_sem.at[0], 1)
                pl.semaphore_signal(
                    far_sem.at[1], inc=1, device_id=(me, row_size - 1), device_id_type=MESH
                )

    def tell_left():
        @pl.when(row == row_size - 1)
        def _():
            pl.semaphore_wait(far_sem.at[1], 1)
            greet(me > 0, near_sem.at[0], (me - 1, row))
            greet(last, near_sem.at[1], right_id)

    def tell_right():
        @pl.when(jnp.logical_and(row == row_size - 1, me < grp_size - 1))
        def _():
            pl.semaphore_wait(near_sem.at[0], 1)
            pl.semaphore_signal(
                near_sem.at[1], inc=1, device_id=right_id, device_id_type=MESH
            )

    def send_rest():
        for h in range(PARTS):
            for i in range(1, grp_size):
                ok = me + i < grp_size - 1
                if h < PARTS // 2:
                    ok = jnp.logical_and(ok, row == row_size - 1)
                pl.when(ok)(arrivals[h, i].start)

    for copy in small_copies:
        copy.wait()

    grp_iota = lax.broadcasted_iota(jnp.int32, (grp_size, elems), 0)
    named = [
        jnp.where(owner_v[c] == grp_iota, np.float32(1), np.float32(0)) for c in range(4)
    ]
    before = (
        lax.broadcasted_iota(jnp.int32, (elems, elems), 0)
        < lax.broadcasted_iota(jnp.int32, (elems, elems), 1)
    )
    running = jnp.dot(
        (named[0] + named[1] + named[2] + named[3]).astype(jnp.bfloat16),
        jnp.where(before, np.float32(1), np.float32(0)).astype(jnp.bfloat16),
        preferred_element_type=jnp.float32,
    )
    targets = []
    for c in range(4):
        rank = jnp.sum(named[c] * running, axis=0, keepdims=True).astype(jnp.int32)
        running = running + named[c]
        slot = me - owner_v[c]
        slot = jnp.where(slot < 0, slot + grp_size, slot)
        targets.append(slot * cap + rank)

    blocks = [jnp.broadcast_to(t // LANES, (2 * part, elems)) for t in targets]
    places = [jnp.broadcast_to(t % LANES, (2 * part, elems)) for t in targets]

    halves = half_weights()
    width = fields * nodes
    lane = lax.broadcasted_iota(jnp.int32, (fields, width), 1)
    spread = jnp.where(
        lane // nodes == lax.broadcasted_iota(jnp.int32, (fields, width), 0),
        np.float32(1),
        np.float32(0),
    )
    mix = jnp.dot(
        mix_v[...], spread, precision=lax.Precision.HIGHEST, preferred_element_type=jnp.float32
    )
    node = lane % nodes
    row_node = lax.broadcasted_iota(jnp.int32, (nodes, elems), 0)
    metric = metric_v[...]
    rows, scales = [], []
    for c in range(4):
        a, b = c % 2, c // 2
        rows.append(mix * pick(node % 4, halves[a]) * pick(node // 4, halves[b]))
        weights = pick(row_node % 4, halves[a]) * pick(row_node // 4, halves[b])
        area = jnp.sum(weights * metric, axis=0, keepdims=True)
        scales.append(jnp.broadcast_to(1.0 / area, (fields, elems)))
    scale = jnp.concatenate(scales, axis=0)
    high, low = split(jnp.concatenate(rows, axis=0))
    matrix = jnp.concatenate(
        [
            jnp.concatenate([high, high], axis=1),
            jnp.concatenate([low, jnp.zeros_like(low)], axis=1),
        ],
        axis=0,
    )
    count = 4 * fields

    def weigh(level):
        x = (gll_v[:, level] * metric[None]).reshape(width, elems)
        return jnp.concatenate(split(x), axis=0)

    send_later(1)
    for k in range(chunks):
        gll_copies[k].wait()

        def remap(j, carry):
            level = k * chunk + 2 * j
            data = jnp.concatenate([weigh(level), weigh(level + 1)], axis=1)
            out = jnp.dot(matrix, data, preferred_element_type=jnp.float32)
            out = out[:count] + out[count:]
            mixed_v[level] = out[:, :elems] * scale
            mixed_v[level + 1] = out[:, elems:] * scale
            return carry

        lax.fori_loop(0, chunk // 2, remap, 0, unroll=True)
        if k + 2 < grp_size:
            send_later(k + 2)
        if k == 0:
            tell_left()
    tell_right()

    for i in range(chunks + 2, grp_size):
        send_later(i)
    send_rest()

    quarter = lax.broadcasted_iota(jnp.int32, (fields, elems), 1) // HALO
    hear(jnp.logical_and(odd, row < row_size - 1), near_sem.at[0])
    hear(jnp.logical_or(jnp.logical_and(odd, row != 1), row == 0), near_sem.at[1])
    halo_copies = []
    for h in range(PARTS):
        picked = [None] * 4
        whole = recv_v.at[h]
        pltpu.make_async_copy(whole, whole, recv_sem.at[h]).wait()
        for i in range(grp_size):
            if i == 0:
                held = slots_v[h, :, block_of(me)]
            else:
                held = recv_v[h, i - 1]
            for k in range(cap // LANES):
                source = held[:, k * LANES : (k + 1) * LANES]
                for c in range(4):
                    value = jnp.take_along_axis(
                        source, places[c], axis=1, mode="promise_in_bounds"
                    )
                    if picked[c] is None:
                        picked[c] = value
                    else:
                        block = i * (cap // LANES) + k
                        picked[c] = jnp.where(blocks[c] == block, value, picked[c])
        for c in range(4):
            sel_v[h, c] = picked[c]
        for q in range(packs):
            to_right = to_left = None
            for p in range(pack):
                at = q * pack + p
                level = h * part + at
                mean = None
                for c in range(4):
                    span = pl.ds(c * fields, fields)
                    tend = sel_v[h, c, pl.ds(at, 1)] * jnp.tanh(
                        mixed_v[level, span] + sel_v[h, c, pl.ds(part + at, 1)]
                    )
                    if h == PARTS - 1:
                        tail_ref[at, span] = tend
                    else:
                        tend_v[level, span] = tend
                    mean = tend if mean is None else mean + tend
                mean = mean * np.float32(0.25)
                to_r = pltpu.roll(mean, (HALO * (p + 1)) % elems, 1) if (p + 1) % pack else mean
                to_l = pltpu.roll(mean, HALO * p, 1) if p else mean
                to_right = to_r if p == 0 else jnp.where(quarter == p, to_r, to_right)
                to_left = to_l if p == 0 else jnp.where(quarter == p, to_l, to_left)
            pack_v[0, h * packs + q] = to_right
            pack_v[1, h * packs + q] = to_left
        span = pl.ds(h * packs, packs)
        for way, device in ((0, right_id), (1, left_id)):
            copy = pltpu.make_async_remote_copy(
                src_ref=pack_v.at[way, span],
                dst_ref=halo_v.at[way, span],
                send_sem=halo_send_sem.at[h, way],
                recv_sem=halo_recv_sem.at[h, way],
                device_id=device,
                device_id_type=MESH,
            )
            copy.start()
            halo_copies.append(copy)

    pltpu.make_async_copy(recv_v, recv_v, send_sem).wait()
    write = nodes_writer(row_size, neighbours_v[...], fields, elems)
    for h in range(PARTS - 1):
        halo_copies[2 * h].wait()
        halo_copies[2 * h + 1].wait()

        def group(q, carry):
            for p in range(pack):
                level = q * pack + p

                def store(f, v, value):
                    done_ref[f, level, pl.ds(8 * v, 8), :] = value

                write(
                    tend_v.at[level], halo_v[0, q], halo_v[1, q], p, work_v.at[p], store
                )
            return carry

        lax.fori_loop(h * packs, (h + 1) * packs, group, 0)
    for copy in halo_copies[2 * PARTS - 2 :]:
        copy.wait()
    for way in range(2):
        for q in range(packs):
            tail_halo_ref[way, q] = halo_v[way, levels // pack - packs + q]


def last_part_kernel(
    row_size, done_ref, tend_ref, halo_ref, neighbours_ref, out_ref, last_v, work_v, sem
):
    fields, part, nodes, elems = last_v.shape
    pack = elems // HALO
    before = done_ref.shape[1]
    copies = []
    for k in range(before // part):
        span = pl.ds(k * part, part)
        copy = pltpu.make_async_copy(done_ref.at[:, span], out_ref.at[:, span], sem.at[k])
        copy.start()
        copies.append(copy)
    write = nodes_writer(row_size, neighbours_ref[...], fields, elems)
    for q in range(part // pack):
        for p in range(pack):
            level = q * pack + p

            def store(f, v, value):
                last_v[f, level, pl.ds(8 * v, 8), :] = value

            write(
                tend_ref.at[level], halo_ref[0, q], halo_ref[1, q], p, work_v.at[level], store
            )
        copy = pltpu.make_async_copy(
            last_v.at[:, pl.ds(q * pack, pack)],
            out_ref.at[:, pl.ds(before + q * pack, pack)],
            sem.at[before // part + q],
        )
        copy.start()
        copies.append(copy)
    for copy in copies:
        copy.wait()


def on_device(gll_state, metric, phys_owner, neighbours, phys_rate, phys_forcing, field_mix):
    fields, levels, nodes, elems = gll_state.shape
    grp_size = lax.axis_size("grp")
    row_size = lax.axis_size("row")
    capacity = phys_rate.shape[1] // grp_size
    cap = -(-capacity // 128) * 128
    if cap != capacity:
        phys_rate, phys_forcing = (
            jnp.pad(
                x.reshape(levels, grp_size, capacity), ((0, 0), (0, 0), (0, cap - capacity))
            ).reshape(levels, grp_size * cap)
            for x in (phys_rate, phys_forcing)
        )
    owner = phys_owner.transpose(1, 2, 0)
    pack = elems // HALO
    part = levels // PARTS
    chunks = 4
    vmem = pl.BlockSpec(memory_space=pltpu.VMEM)
    hbm = pl.BlockSpec(memory_space=pltpu.HBM)
    before = levels - part
    done, tail, tail_halo = pl.pallas_call(
        functools.partial(exchange_kernel, grp_size, row_size),
        out_shape=(
            jax.ShapeDtypeStruct((fields, before, nodes, elems), jnp.float32),
            jax.ShapeDtypeStruct((part, 4 * fields, elems), jnp.float32),
            jax.ShapeDtypeStruct((2, part // pack, fields, elems), jnp.float32),
        ),
        in_specs=[hbm] * 7,
        out_specs=(vmem, vmem, vmem),
        scratch_shapes=[
            pltpu.VMEM((fields, levels, nodes, elems), jnp.float32),
            pltpu.VMEM((nodes, elems), jnp.float32),
            pltpu.VMEM((4, 1, elems), jnp.int32),
            pltpu.VMEM((fields, fields), jnp.float32),
            pltpu.VMEM((4, elems), jnp.int32),
            pltpu.VMEM((PARTS, 2 * part, grp_size * cap), jnp.float32),
            pltpu.VMEM((levels, 4 * fields, elems), jnp.float32),
            pltpu.VMEM((PARTS, grp_size - 1, 2 * part, cap), jnp.float32),
            pltpu.VMEM((PARTS, 4, 2 * part, elems), jnp.float32),
            pltpu.VMEM((before, 4 * fields, elems), jnp.float32),
            pltpu.VMEM((2, levels // pack, fields, elems), jnp.float32),
            pltpu.VMEM((2, levels // pack, fields, elems), jnp.float32),
            pltpu.VMEM((pack, 6, fields, elems), jnp.float32),
            pltpu.SemaphoreType.DMA((chunks,)),
            pltpu.SemaphoreType.DMA((4,)),
            pltpu.SemaphoreType.DMA((PARTS, 2)),
            pltpu.SemaphoreType.DMA,
            pltpu.SemaphoreType.DMA((PARTS,)),
            pltpu.SemaphoreType.DMA((PARTS, 2)),
            pltpu.SemaphoreType.DMA((PARTS, 2)),
            pltpu.SemaphoreType.REGULAR((grp_size,)),
            pltpu.SemaphoreType.REGULAR((2,)),
            pltpu.SemaphoreType.REGULAR((2,)),
        ],
        compiler_params=pltpu.CompilerParams(
            collective_id=0, has_side_effects=True, vmem_limit_bytes=32 * 1024 * 1024
        ),
        name="exchange",
    )(
        *(
            pltpu.with_memory_space_constraint(x, pltpu.HBM)
            for x in (
                gll_state,
                metric,
                owner,
                phys_rate,
                phys_forcing,
                field_mix,
                neighbours,
            )
        )
    )
    anywhere = pl.BlockSpec(memory_space=pl.ANY)
    return pl.pallas_call(
        functools.partial(last_part_kernel, row_size),
        out_shape=jax.ShapeDtypeStruct(gll_state.shape, jnp.float32),
        in_specs=[anywhere, vmem, vmem, vmem],
        out_specs=anywhere,
        scratch_shapes=[
            pltpu.VMEM((fields, part, nodes, elems), jnp.float32),
            pltpu.VMEM((part, 6, fields, elems), jnp.float32),
            pltpu.SemaphoreType.DMA((PARTS - 1 + part // pack,)),
        ],
        compiler_params=pltpu.CompilerParams(vmem_limit_bytes=16 * 1024 * 1024),
        name="last_part",
    )(done, tail, tail_halo, neighbours)


def solution(mesh):
    in_specs = (
        P(None, None, None, ("grp", "row")),
        P(None, ("grp", "row")),
        P(("grp", "row"), None, None),
        P(None, ("grp", "row")),
        P(None, ("grp", "row")),
        P(None, ("grp", "row")),
        P(),
    )
    out_specs = P(None, None, None, ("grp", "row"))
    return jax.shard_map(
        on_device, mesh=mesh, in_specs=in_specs, out_specs=out_specs, check_vma=False
    )
```

```python
import functools

import jax
import jax.numpy as jnp
import numpy as np
from jax import lax
from jax.experimental import pallas as pl
from jax.experimental.pallas import tpu as pltpu
from jax.sharding import PartitionSpec as P

HALO = 32
MESH = pl.DeviceIdType.MESH
PARTS = 4
LANES = 128
GLL = [-1.0, -1.0 / np.sqrt(5.0), 1.0 / np.sqrt(5.0), 1.0]


def half_weights():
    offset = 0.5 / np.sqrt(3.0)
    halves = np.zeros((2, 4))
    for i in range(4):
        for a, middle in enumerate((-0.5, 0.5)):
            for point in (middle - offset, middle + offset):
                value = 0.5
                for k in range(4):
                    if k != i:
                        value *= (point - GLL[k]) / (GLL[i] - GLL[k])
                halves[a, i] += value
    return halves


def pick(index, values):
    out = jnp.full(index.shape, np.float32(values[-1]), jnp.float32)
    for k in range(len(values) - 1):
        out = jnp.where(index == k, np.float32(values[k]), out)
    return out


def split(x):
    high = x.astype(jnp.bfloat16)
    low = (x - high.astype(jnp.float32)).astype(jnp.bfloat16)
    return high, low


def nodes_writer(row_size, neighbours, fields, elems):
    flat = lax.axis_index("grp") * row_size + lax.axis_index("row")
    inside, places = [], []
    for k in range(4):
        spot = neighbours[k : k + 1] - flat * elems
        within = jnp.where((spot >= 0) & (spot < elems), 1, 0)
        inside.append(jnp.broadcast_to(within, (fields, elems)) == 1)
        places.append(jnp.broadcast_to(neighbours[k : k + 1] % elems, (fields, elems)))
    lane = lax.broadcasted_iota(jnp.int32, (fields, elems), 1)
    sub = lax.broadcasted_iota(jnp.int32, (8, elems), 0)
    gi = pick(sub % 4, GLL)
    gj = [pick(sub // 4, GLL[:2]), pick(sub // 4, GLL[2:])]
    left_x, right_x = 0.5 - gi, 0.5 + gi
    low_y = [0.5 - g for g in gj]
    high_y = [0.5 + g for g in gj]
    slope_left = 0.5 * jnp.maximum(0.0, -gi)
    slope_right = 0.5 * jnp.maximum(0.0, gi)
    slope_y = [0.5 * jnp.maximum(0.0, -gj[0]), 0.5 * jnp.maximum(0.0, gj[1])]

    def take(x, index):
        return jnp.take_along_axis(x, index, axis=1, mode="promise_in_bounds")

    def write(tend_ref, from_left, from_right, p, work_ref, store):
        cells = [tend_ref[pl.ds(c * fields, fields), :] for c in range(4)]
        own = (cells[0] + cells[1] + cells[2] + cells[3]) * np.float32(0.25)
        from_left = pltpu.roll(from_left, (elems - HALO * (p + 1)) % elems, 1)
        if p:
            from_right = pltpu.roll(from_right, elems - HALO * p, 1)
        halo = jnp.where(lane < elems // 2, from_right, from_left)
        around = [
            jnp.where(inside[k], take(own, places[k]), take(halo, places[k])) for k in range(4)
        ]
        low = functools.reduce(jnp.minimum, cells + around)
        high = functools.reduce(jnp.maximum, cells + around)
        for k in range(4):
            work_ref[k] = around[k] - own
        work_ref[4] = low
        work_ref[5] = high
        for f in range(fields):
            cell = [tend_ref[pl.ds(c * fields + f, 1), :] for c in range(4)]
            west, east, south, north, lower, upper = (
                work_ref[k, pl.ds(f, 1), :] for k in range(6)
            )
            bottom = left_x * cell[0] + right_x * cell[1]
            top = left_x * cell[2] + right_x * cell[3]
            slope = slope_left * west + slope_right * east
            for v, side in ((0, south), (1, north)):
                value = low_y[v] * bottom + high_y[v] * top + (slope + slope_y[v] * side)
                store(f, v, jnp.minimum(jnp.maximum(value, lower), upper))

    return write


def exchange_kernel(
    grp_size,
    row_size,
    gll_ref,
    metric_ref,
    owner_ref,
    rate_ref,
    forcing_ref,
    mix_ref,
    neighbours_ref,
    done_ref,
    tail_ref,
    tail_halo_ref,
    gll_v,
    metric_v,
    owner_v,
    mix_v,
    neighbours_v,
    slots_v,
    mixed_v,
    recv_v,
    sel_v,
    tend_v,
    pack_v,
    halo_v,
    work_v,
    gll_sem,
    small_sem,
    slots_sem,
    send_sem,
    recv_sem,
    halo_send_sem,
    halo_recv_sem,
    ready_sem,
    near_sem,
    far_sem,
    relay_v,
    relay_send_sem,
    relay_recv_sem,
):
    fields, levels, nodes, elems = gll_v.shape
    part = levels // PARTS
    cap = recv_v.shape[3]

    def block_of(peer):
        return pl.ds(pl.multiple_of(peer * cap, cap), cap)

    chunks = gll_sem.shape[0]
    chunk = levels // chunks
    pack = elems // HALO
    packs = part // pack
    me = lax.axis_index("grp")
    row = lax.axis_index("row")
    flat = me * row_size + row
    total = grp_size * row_size
    right = lax.rem(flat + 1, total)
    left = lax.rem(flat + total - 1, total)
    right_id = (right // row_size, lax.rem(right, row_size))
    left_id = (left // row_size, lax.rem(left, row_size))

    barrier = pltpu.get_barrier_semaphore()
    first, last = flat == 0, flat == total - 1

    def greet(when, semaphore, device):
        @pl.when(when)
        def _():
            pl.semaphore_signal(semaphore, inc=1, device_id=device, device_id_type=MESH)

    def hear(when, semaphore):
        @pl.when(when)
        def _():
            pl.semaphore_wait(semaphore, 1)

    wide = 2 if grp_size % 2 == 0 else 1
    deep, side = me // wide, lax.rem(me, wide)
    even = lax.rem(row, 2) == 0
    slot_copies = []
    for h in range(PARTS):
        for kind, ref in enumerate((rate_ref, forcing_ref)):
            copy = pltpu.make_async_copy(
                ref.at[pl.ds(h * part, part)],
                slots_v.at[h, pl.ds(kind * part, part)],
                slots_sem.at[h, kind],
            )
            copy.start()
            slot_copies.append(copy)
    for peer in range(1, grp_size):
        greet(
            jnp.logical_and(peer > me, side <= peer % wide), barrier, (peer, row)
        )
    odd = jnp.logical_not(even)
    greet(odd, barrier, (me, row - 1))
    greet(jnp.logical_and(odd, row < row_size - 1), barrier, (me, row + 1))
    greet(row == 1, barrier, (me, row_size - 1))

    small_copies = []
    for k, (src, dst) in enumerate(
        (
            (owner_ref, owner_v),
            (metric_ref, metric_v),
            (mix_ref, mix_v),
            (neighbours_ref, neighbours_v),
        )
    ):
        copy = pltpu.make_async_copy(src, dst, small_sem.at[k])
        copy.start()
        small_copies.append(copy)
    gll_copies = []
    for k in range(chunks):
        span = pl.ds(k * chunk, chunk)
        copy = pltpu.make_async_copy(gll_ref.at[:, span], gll_v.at[:, span], gll_sem.at[k])
        copy.start()
        gll_copies.append(copy)

    def count(*conditions):
        return sum(jnp.where(c, 1, 0) for c in conditions)

    heard = (
        (deep + 1) * (side + 1)
        - 1
        + count(even, jnp.logical_and(even, row > 0), row == row_size - 1)
    )

    @pl.when(heard > 0)
    def _():
        pl.semaphore_wait(barrier, heard)

    for peer in range(grp_size - 1):
        greet(
            jnp.logical_and(peer < me, peer % wide <= side), ready_sem.at[me], (peer, row)
        )
    greet(jnp.logical_and(even, row > 0), near_sem.at[0], (me, row - 1))
    greet(even, near_sem.at[1], (me, row + 1))
    greet(row == row_size - 1, far_sem.at[0], (me, 1))

    arrivals = {}
    for h in range(PARTS):
        for i in range(1, grp_size):
            peer = lax.rem(me + i, grp_size)
            arrivals[h, i] = pltpu.make_async_remote_copy(
                src_ref=slots_v.at[h, :, block_of(peer)],
                dst_ref=recv_v.at[h, i - 1],
                send_sem=send_sem,
                recv_sem=recv_sem.at[h],
                device_id=(peer, row),
                device_id_type=MESH,
            )
    for copy in slot_copies:
        copy.wait()

    def send_to(j, parts, when):
        @pl.when(jnp.logical_and(j < me, when))
        def _():
            i = j + grp_size - me
            for h in parts:
                pltpu.make_async_remote_copy(
                    src_ref=slots_v.at[h, :, pl.ds(j * cap, cap)],
                    dst_ref=recv_v.at[h, i - 1],
                    send_sem=send_sem,
                    recv_sem=recv_sem.at[h],
                    device_id=(j, row),
                    device_id_type=MESH,
                ).start()

    def send_back(allowed, parts, when):
        for j in range(grp_size // 4):
            if allowed(j):
                send_to(j, parts, when(j))
        for some in (parts[: len(parts) // 2], parts[len(parts) // 2 :]):
            for j in range(grp_size // 4, grp_size - 1):
                if some and allowed(j):
                    send_to(j, some, when(j))

    every = list(range(PARTS))
    send_back(lambda j: True, every, lambda j: side >= j % wide)

    far_first = row == row_size - 1
    hop = grp_size // (4 * wide) * wide
    relays = jnp.logical_and(me >= hop, me < 2 * hop)

    def send_one(i, when):
        @pl.when(
            jnp.logical_and(
                jnp.logical_and(when, me + i < grp_size), jnp.logical_not(far_first)
            )
        )
        def _():
            for h in range(PARTS // 2):
                arrivals[h, i].start()

        @pl.when(
            jnp.logical_and(
                jnp.logical_and(when, me + i == grp_size - 1),
                jnp.logical_and(far_first, me >= hop),
            )
        )
        def _():
            for h in range(PARTS):
                arrivals[h, i].start()

        if i < grp_size - hop:
            @pl.when(
                jnp.logical_and(
                    jnp.logical_and(when, me + i == grp_size - 1),
                    jnp.logical_and(far_first, relays),
                )
            )
            def _():
                for h in range(PARTS):
                    held = relay_v.at[h]
                    pltpu.make_async_copy(held, held, relay_recv_sem.at[h]).wait()
                    pltpu.make_async_remote_copy(
                        src_ref=held,
                        dst_ref=recv_v.at[h, i + hop - 1],
                        send_sem=relay_send_sem,
                        recv_sem=recv_sem.at[h],
                        device_id=(grp_size - 1, row),
                        device_id_type=MESH,
                    ).start()

    def hand_over():
        for h in range(PARTS):
            pltpu.make_async_remote_copy(
                src_ref=slots_v.at[h, :, block_of(grp_size - 1)],
                dst_ref=relay_v.at[h],
                send_sem=send_sem,
                recv_sem=relay_recv_sem.at[h],
                device_id=(me + hop, row),
                device_id_type=MESH,
            ).start()

    def send_later(i):
        above = jnp.logical_and(me + i < grp_size, lax.rem(me + i, wide) >= side)

        @pl.when(above)
        def _():
            pl.semaphore_wait(ready_sem.at[me + i], 1)

        if wide == 2 and i % 2 == 0:
            send_one(i - 1, jnp.logical_and(above, side == 1))
        if i == hop:
            pl.when(jnp.logical_and(far_first, me < hop))(hand_over)
        send_one(i, above)
        if i == 1:
            if wide == 2:
                send_back(lambda j: j % wide == 1, every, lambda j: side == 0)

            @pl.when(row == 1)
            def _():
                pl.semaphore_wait(near_sem.at[1], 1)
                pl.semaphore_wait(far_sem.at[0], 1)
                pl.semaphore_signal(
                    far_sem.at[1], inc=1, device_id=(me, row_size - 1), device_id_type=MESH
                )

    def tell_left():
        @pl.when(row == row_size - 1)
        def _():
            pl.semaphore_wait(far_sem.at[1], 1)
            greet(me > 0, near_sem.at[0], (me - 1, row))
            greet(last, near_sem.at[1], right_id)

    def tell_right():
        @pl.when(jnp.logical_and(row == row_size - 1, me < grp_size - 1))
        def _():
            pl.semaphore_wait(near_sem.at[0], 1)
            pl.semaphore_signal(
                near_sem.at[1], inc=1, device_id=right_id, device_id_type=MESH
            )

    def send_rest():
        for some in (range(PARTS // 2), range(PARTS // 2, PARTS)):
            for i in range(1, grp_size):
                ok = me + i < grp_size - 1
                if some[0] == 0:
                    ok = jnp.logical_and(ok, far_first)
                else:
                    ok = jnp.logical_or(
                        ok, jnp.logical_and(me + i == grp_size - 1, jnp.logical_not(far_first))
                    )

                @pl.when(ok)
                def _():
                    for h in some:
                        arrivals[h, i].start()

    for copy in small_copies:
        copy.wait()

    grp_iota = lax.broadcasted_iota(jnp.int32, (grp_size, elems), 0)
    named = [
        jnp.where(owner_v[c] == grp_iota, np.float32(1), np.float32(0)) for c in range(4)
    ]
    before = (
        lax.broadcasted_iota(jnp.int32, (elems, elems), 0)
        < lax.broadcasted_iota(jnp.int32, (elems, elems), 1)
    )
    running = jnp.dot(
        (named[0] + named[1] + named[2] + named[3]).astype(jnp.bfloat16),
        jnp.where(before, np.float32(1), np.float32(0)).astype(jnp.bfloat16),
        preferred_element_type=jnp.float32,
    )
    targets = []
    for c in range(4):
        rank = jnp.sum(named[c] * running, axis=0, keepdims=True).astype(jnp.int32)
        running = running + named[c]
        slot = me - owner_v[c]
        slot = jnp.where(slot < 0, slot + grp_size, slot)
        targets.append(slot * cap + rank)

    blocks = [jnp.broadcast_to(t // LANES, (2 * part, elems)) for t in targets]
    places = [jnp.broadcast_to(t % LANES, (2 * part, elems)) for t in targets]

    halves = half_weights()
    width = fields * nodes
    lane = lax.broadcasted_iota(jnp.int32, (fields, width), 1)
    spread = jnp.where(
        lane // nodes == lax.broadcasted_iota(jnp.int32, (fields, width), 0),
        np.float32(1),
        np.float32(0),
    )
    mix = jnp.dot(
        mix_v[...], spread, precision=lax.Precision.HIGHEST, preferred_element_type=jnp.float32
    )
    node = lane % nodes
    row_node = lax.broadcasted_iota(jnp.int32, (nodes, elems), 0)
    metric = metric_v[...]
    rows, scales = [], []
    for c in range(4):
        a, b = c % 2, c // 2
        rows.append(mix * pick(node % 4, halves[a]) * pick(node // 4, halves[b]))
        weights = pick(row_node % 4, halves[a]) * pick(row_node // 4, halves[b])
        area = jnp.sum(weights * metric, axis=0, keepdims=True)
        scales.append(jnp.broadcast_to(1.0 / area, (fields, elems)))
    scale = jnp.concatenate(scales, axis=0)
    high, low = split(jnp.concatenate(rows, axis=0))
    matrix = jnp.concatenate(
        [
            jnp.concatenate([high, high], axis=1),
            jnp.concatenate([low, jnp.zeros_like(low)], axis=1),
        ],
        axis=0,
    )
    count = 4 * fields

    def weigh(level):
        x = (gll_v[:, level] * metric[None]).reshape(width, elems)
        return jnp.concatenate(split(x), axis=0)

    send_later(1)
    send_later(2)
    for k in range(chunks):
        gll_copies[k].wait()

        def remap(j, carry):
            level = k * chunk + 2 * j
            data = jnp.concatenate([weigh(level), weigh(level + 1)], axis=1)
            out = jnp.dot(matrix, data, preferred_element_type=jnp.float32)
            out = out[:count] + out[count:]
            mixed_v[level] = out[:, :elems] * scale
            mixed_v[level + 1] = out[:, elems:] * scale
            return carry

        lax.fori_loop(0, chunk // 2, remap, 0, unroll=True)
        if k + 3 < grp_size:
            send_later(k + 3)
        if k == 0:
            tell_left()
    tell_right()

    for i in range(chunks + 3, grp_size):
        send_later(i)
    send_rest()

    quarter = lax.broadcasted_iota(jnp.int32, (fields, elems), 1) // HALO
    hear(jnp.logical_and(odd, row < row_size - 1), near_sem.at[0])
    hear(jnp.logical_or(jnp.logical_and(odd, row != 1), row == 0), near_sem.at[1])
    halo_copies = []
    for h in range(PARTS):
        picked = [None] * 4
        whole = recv_v.at[h]
        pltpu.make_async_copy(whole, whole, recv_sem.at[h]).wait()
        for i in range(grp_size):
            if i == 0:
                held = slots_v[h, :, block_of(me)]
            else:
                held = recv_v[h, i - 1]
            for k in range(cap // LANES):
                source = held[:, k * LANES : (k + 1) * LANES]
                for c in range(4):
                    value = jnp.take_along_axis(
                        source, places[c], axis=1, mode="promise_in_bounds"
                    )
                    if picked[c] is None:
                        picked[c] = value
                    else:
                        block = i * (cap // LANES) + k
                        picked[c] = jnp.where(blocks[c] == block, value, picked[c])
        for c in range(4):
            sel_v[h, c] = picked[c]
        for q in range(packs):
            to_right = to_left = None
            for p in range(pack):
                at = q * pack + p
                level = h * part + at
                mean = None
                for c in range(4):
                    span = pl.ds(c * fields, fields)
                    tend = sel_v[h, c, pl.ds(at, 1)] * jnp.tanh(
                        mixed_v[level, span] + sel_v[h, c, pl.ds(part + at, 1)]
                    )
                    if h == PARTS - 1:
                        tail_ref[at, span] = tend
                    else:
                        tend_v[level, span] = tend
                    mean = tend if mean is None else mean + tend
                mean = mean * np.float32(0.25)
                to_r = pltpu.roll(mean, (HALO * (p + 1)) % elems, 1) if (p + 1) % pack else mean
                to_l = pltpu.roll(mean, HALO * p, 1) if p else mean
                to_right = to_r if p == 0 else jnp.where(quarter == p, to_r, to_right)
                to_left = to_l if p == 0 else jnp.where(quarter == p, to_l, to_left)
            pack_v[0, h * packs + q] = to_right
            pack_v[1, h * packs + q] = to_left
        span = pl.ds(h * packs, packs)
        for way, device in ((0, right_id), (1, left_id)):
            copy = pltpu.make_async_remote_copy(
                src_ref=pack_v.at[way, span],
                dst_ref=halo_v.at[way, span],
                send_sem=halo_send_sem.at[h, way],
                recv_sem=halo_recv_sem.at[h, way],
                device_id=device,
                device_id_type=MESH,
            )
            copy.start()
            halo_copies.append(copy)

    pltpu.make_async_copy(recv_v, recv_v, send_sem).wait()

    @pl.when(jnp.logical_and(far_first, relays))
    def _():
        pltpu.make_async_copy(relay_v, relay_v, relay_send_sem).wait()

    write = nodes_writer(row_size, neighbours_v[...], fields, elems)
    for h in range(PARTS - 1):
        halo_copies[2 * h].wait()
        halo_copies[2 * h + 1].wait()

        def group(q, carry):
            for p in range(pack):
                level = q * pack + p

                def store(f, v, value):
                    done_ref[f, level, pl.ds(8 * v, 8), :] = value

                write(
                    tend_v.at[level], halo_v[0, q], halo_v[1, q], p, work_v.at[p], store
                )
            return carry

        lax.fori_loop(h * packs, (h + 1) * packs, group, 0, unroll=True)
    for copy in halo_copies[2 * PARTS - 2 :]:
        copy.wait()
    for way in range(2):
        for q in range(packs):
            tail_halo_ref[way, q] = halo_v[way, levels // pack - packs + q]


def last_part_kernel(
    row_size, done_ref, tend_ref, halo_ref, neighbours_ref, out_ref, last_v, work_v, sem
):
    fields, part, nodes, elems = last_v.shape
    pack = elems // HALO
    before = done_ref.shape[1]
    copies = []
    for k in range(before // part):
        span = pl.ds(k * part, part)
        copy = pltpu.make_async_copy(done_ref.at[:, span], out_ref.at[:, span], sem.at[k])
        copy.start()
        copies.append(copy)
    write = nodes_writer(row_size, neighbours_ref[...], fields, elems)
    for q in range(part // pack):
        for p in range(pack):
            level = q * pack + p

            def store(f, v, value):
                last_v[f, level, pl.ds(8 * v, 8), :] = value

            write(
                tend_ref.at[level], halo_ref[0, q], halo_ref[1, q], p, work_v.at[level], store
            )
        copy = pltpu.make_async_copy(
            last_v.at[:, pl.ds(q * pack, pack)],
            out_ref.at[:, pl.ds(before + q * pack, pack)],
            sem.at[before // part + q],
        )
        copy.start()
        copies.append(copy)
    for copy in copies:
        copy.wait()


def on_device(gll_state, metric, phys_owner, neighbours, phys_rate, phys_forcing, field_mix):
    fields, levels, nodes, elems = gll_state.shape
    grp_size = lax.axis_size("grp")
    row_size = lax.axis_size("row")
    capacity = phys_rate.shape[1] // grp_size
    cap = -(-capacity // 128) * 128
    if cap != capacity:
        phys_rate, phys_forcing = (
            jnp.pad(
                x.reshape(levels, grp_size, capacity), ((0, 0), (0, 0), (0, cap - capacity))
            ).reshape(levels, grp_size * cap)
            for x in (phys_rate, phys_forcing)
        )
    owner = phys_owner.transpose(1, 2, 0)
    pack = elems // HALO
    part = levels // PARTS
    chunks = 4
    vmem = pl.BlockSpec(memory_space=pltpu.VMEM)
    hbm = pl.BlockSpec(memory_space=pltpu.HBM)
    before = levels - part
    done, tail, tail_halo = pl.pallas_call(
        functools.partial(exchange_kernel, grp_size, row_size),
        out_shape=(
            jax.ShapeDtypeStruct((fields, before, nodes, elems), jnp.float32),
            jax.ShapeDtypeStruct((part, 4 * fields, elems), jnp.float32),
            jax.ShapeDtypeStruct((2, part // pack, fields, elems), jnp.float32),
        ),
        in_specs=[hbm] * 7,
        out_specs=(vmem, vmem, vmem),
        scratch_shapes=[
            pltpu.VMEM((fields, levels, nodes, elems), jnp.float32),
            pltpu.VMEM((nodes, elems), jnp.float32),
            pltpu.VMEM((4, 1, elems), jnp.int32),
            pltpu.VMEM((fields, fields), jnp.float32),
            pltpu.VMEM((4, elems), jnp.int32),
            pltpu.VMEM((PARTS, 2 * part, grp_size * cap), jnp.float32),
            pltpu.VMEM((levels, 4 * fields, elems), jnp.float32),
            pltpu.VMEM((PARTS, grp_size - 1, 2 * part, cap), jnp.float32),
            pltpu.VMEM((PARTS, 4, 2 * part, elems), jnp.float32),
            pltpu.VMEM((before, 4 * fields, elems), jnp.float32),
            pltpu.VMEM((2, levels // pack, fields, elems), jnp.float32),
            pltpu.VMEM((2, levels // pack, fields, elems), jnp.float32),
            pltpu.VMEM((pack, 6, fields, elems), jnp.float32),
            pltpu.SemaphoreType.DMA((chunks,)),
            pltpu.SemaphoreType.DMA((4,)),
            pltpu.SemaphoreType.DMA((PARTS, 2)),
            pltpu.SemaphoreType.DMA,
            pltpu.SemaphoreType.DMA((PARTS,)),
            pltpu.SemaphoreType.DMA((PARTS, 2)),
            pltpu.SemaphoreType.DMA((PARTS, 2)),
            pltpu.SemaphoreType.REGULAR((grp_size,)),
            pltpu.SemaphoreType.REGULAR((2,)),
            pltpu.SemaphoreType.REGULAR((2,)),
            pltpu.VMEM((PARTS, 2 * part, cap), jnp.float32),
            pltpu.SemaphoreType.DMA,
            pltpu.SemaphoreType.DMA((PARTS,)),
        ],
        compiler_params=pltpu.CompilerParams(
            collective_id=0, has_side_effects=True, vmem_limit_bytes=32 * 1024 * 1024
        ),
        name="exchange",
    )(
        *(
            pltpu.with_memory_space_constraint(x, pltpu.HBM)
            for x in (
                gll_state,
                metric,
                owner,
                phys_rate,
                phys_forcing,
                field_mix,
                neighbours,
            )
        )
    )
    anywhere = pl.BlockSpec(memory_space=pl.ANY)
    return pl.pallas_call(
        functools.partial(last_part_kernel, row_size),
        out_shape=jax.ShapeDtypeStruct(gll_state.shape, jnp.float32),
        in_specs=[anywhere, vmem, vmem, vmem],
        out_specs=anywhere,
        scratch_shapes=[
            pltpu.VMEM((fields, part, nodes, elems), jnp.float32),
            pltpu.VMEM((part, 6, fields, elems), jnp.float32),
            pltpu.SemaphoreType.DMA((PARTS - 1 + part // pack,)),
        ],
        compiler_params=pltpu.CompilerParams(vmem_limit_bytes=16 * 1024 * 1024),
        name="last_part",
    )(done, tail, tail_halo, neighbours)


def solution(mesh):
    in_specs = (
        P(None, None, None, ("grp", "row")),
        P(None, ("grp", "row")),
        P(("grp", "row"), None, None),
        P(None, ("grp", "row")),
        P(None, ("grp", "row")),
        P(None, ("grp", "row")),
        P(),
    )
    out_specs = P(None, None, None, ("grp", "row"))
    return jax.shard_map(
        on_device, mesh=mesh, in_specs=in_specs, out_specs=out_specs, check_vma=False
    )
```

```python
import functools

import jax
import jax.numpy as jnp
import numpy as np
from jax import lax
from jax.experimental import pallas as pl
from jax.experimental.pallas import tpu as pltpu
from jax.sharding import PartitionSpec as P

HALO = 32
MESH = pl.DeviceIdType.MESH
PARTS = 4
LANES = 128
GLL = [-1.0, -1.0 / np.sqrt(5.0), 1.0 / np.sqrt(5.0), 1.0]


def half_weights():
    offset = 0.5 / np.sqrt(3.0)
    halves = np.zeros((2, 4))
    for i in range(4):
        for a, middle in enumerate((-0.5, 0.5)):
            for point in (middle - offset, middle + offset):
                value = 0.5
                for k in range(4):
                    if k != i:
                        value *= (point - GLL[k]) / (GLL[i] - GLL[k])
                halves[a, i] += value
    return halves


def pick(index, values):
    out = jnp.full(index.shape, np.float32(values[-1]), jnp.float32)
    for k in range(len(values) - 1):
        out = jnp.where(index == k, np.float32(values[k]), out)
    return out


def split(x):
    high = x.astype(jnp.bfloat16)
    low = (x - high.astype(jnp.float32)).astype(jnp.bfloat16)
    return high, low


def nodes_writer(row_size, neighbours, fields, elems):
    flat = lax.axis_index("grp") * row_size + lax.axis_index("row")
    inside, places = [], []
    for k in range(4):
        spot = neighbours[k : k + 1] - flat * elems
        within = jnp.where((spot >= 0) & (spot < elems), 1, 0)
        inside.append(jnp.broadcast_to(within, (fields, elems)) == 1)
        places.append(jnp.broadcast_to(neighbours[k : k + 1] % elems, (fields, elems)))
    lane = lax.broadcasted_iota(jnp.int32, (fields, elems), 1)
    sub = lax.broadcasted_iota(jnp.int32, (8, elems), 0)
    gi = pick(sub % 4, GLL)
    gj = [pick(sub // 4, GLL[:2]), pick(sub // 4, GLL[2:])]
    left_x, right_x = 0.5 - gi, 0.5 + gi
    low_y = [0.5 - g for g in gj]
    high_y = [0.5 + g for g in gj]
    slope_left = 0.5 * jnp.maximum(0.0, -gi)
    slope_right = 0.5 * jnp.maximum(0.0, gi)
    slope_y = [0.5 * jnp.maximum(0.0, -gj[0]), 0.5 * jnp.maximum(0.0, gj[1])]

    def take(x, index):
        return jnp.take_along_axis(x, index, axis=1, mode="promise_in_bounds")

    def write(tend_ref, from_left, from_right, p, work_ref, store):
        cells = [tend_ref[pl.ds(c * fields, fields), :] for c in range(4)]
        own = (cells[0] + cells[1] + cells[2] + cells[3]) * np.float32(0.25)
        from_left = pltpu.roll(from_left, (elems - HALO * (p + 1)) % elems, 1)
        if p:
            from_right = pltpu.roll(from_right, elems - HALO * p, 1)
        halo = jnp.where(lane < elems // 2, from_right, from_left)
        around = [
            jnp.where(inside[k], take(own, places[k]), take(halo, places[k])) for k in range(4)
        ]
        low = functools.reduce(jnp.minimum, cells + around)
        high = functools.reduce(jnp.maximum, cells + around)
        for k in range(4):
            work_ref[k] = around[k] - own
        work_ref[4] = low
        work_ref[5] = high
        for f in range(fields):
            cell = [tend_ref[pl.ds(c * fields + f, 1), :] for c in range(4)]
            west, east, south, north, lower, upper = (
                work_ref[k, pl.ds(f, 1), :] for k in range(6)
            )
            bottom = left_x * cell[0] + right_x * cell[1]
            top = left_x * cell[2] + right_x * cell[3]
            slope = slope_left * west + slope_right * east
            for v, side in ((0, south), (1, north)):
                value = low_y[v] * bottom + high_y[v] * top + (slope + slope_y[v] * side)
                store(f, v, jnp.minimum(jnp.maximum(value, lower), upper))

    return write


def exchange_kernel(
    grp_size,
    row_size,
    gll_ref,
    metric_ref,
    owner_ref,
    rate_ref,
    forcing_ref,
    mix_ref,
    neighbours_ref,
    done_ref,
    tail_ref,
    tail_halo_ref,
    gll_v,
    metric_v,
    owner_v,
    mix_v,
    neighbours_v,
    slots_v,
    mixed_v,
    recv_v,
    sel_v,
    tend_v,
    pack_v,
    halo_v,
    work_v,
    gll_sem,
    small_sem,
    slots_sem,
    send_sem,
    recv_sem,
    halo_send_sem,
    halo_recv_sem,
    ready_sem,
    near_sem,
    far_sem,
    relay_v,
    relay_send_sem,
    relay_recv_sem,
):
    fields, levels, nodes, elems = gll_v.shape
    part = levels // PARTS
    cap = recv_v.shape[3]

    def block_of(peer):
        return pl.ds(pl.multiple_of(peer * cap, cap), cap)

    chunks = gll_sem.shape[0]
    chunk = levels // chunks
    pack = elems // HALO
    packs = part // pack
    me = lax.axis_index("grp")
    row = lax.axis_index("row")
    flat = me * row_size + row
    total = grp_size * row_size
    right = lax.rem(flat + 1, total)
    left = lax.rem(flat + total - 1, total)
    right_id = (right // row_size, lax.rem(right, row_size))
    left_id = (left // row_size, lax.rem(left, row_size))

    barrier = pltpu.get_barrier_semaphore()
    first, last = flat == 0, flat == total - 1

    def greet(when, semaphore, device):
        @pl.when(when)
        def _():
            pl.semaphore_signal(semaphore, inc=1, device_id=device, device_id_type=MESH)

    def hear(when, semaphore):
        @pl.when(when)
        def _():
            pl.semaphore_wait(semaphore, 1)

    wide = 2 if grp_size % 2 == 0 else 1
    deep, side = me // wide, lax.rem(me, wide)
    even = lax.rem(row, 2) == 0
    slot_copies = []
    for h in range(PARTS):
        for kind, ref in enumerate((rate_ref, forcing_ref)):
            copy = pltpu.make_async_copy(
                ref.at[pl.ds(h * part, part)],
                slots_v.at[h, pl.ds(kind * part, part)],
                slots_sem.at[h, kind],
            )
            copy.start()
            slot_copies.append(copy)
    for peer in range(1, grp_size):
        greet(
            jnp.logical_and(peer > me, side <= peer % wide), barrier, (peer, row)
        )
    odd = jnp.logical_not(even)
    greet(odd, barrier, (me, row - 1))
    greet(jnp.logical_and(odd, row < row_size - 1), barrier, (me, row + 1))
    greet(row == 1, barrier, (me, row_size - 1))

    small_copies = []
    for k, (src, dst) in enumerate(
        (
            (owner_ref, owner_v),
            (metric_ref, metric_v),
            (mix_ref, mix_v),
            (neighbours_ref, neighbours_v),
        )
    ):
        copy = pltpu.make_async_copy(src, dst, small_sem.at[k])
        copy.start()
        small_copies.append(copy)
    gll_copies = []
    for k in range(chunks):
        span = pl.ds(k * chunk, chunk)
        copy = pltpu.make_async_copy(gll_ref.at[:, span], gll_v.at[:, span], gll_sem.at[k])
        copy.start()
        gll_copies.append(copy)

    def count(*conditions):
        return sum(jnp.where(c, 1, 0) for c in conditions)

    heard = (
        (deep + 1) * (side + 1)
        - 1
        + count(even, jnp.logical_and(even, row > 0), row == row_size - 1)
    )

    @pl.when(heard > 0)
    def _():
        pl.semaphore_wait(barrier, heard)

    for peer in range(grp_size - 1):
        greet(
            jnp.logical_and(peer < me, peer % wide <= side), ready_sem.at[me], (peer, row)
        )
    greet(jnp.logical_and(even, row > 0), near_sem.at[0], (me, row - 1))
    greet(even, near_sem.at[1], (me, row + 1))
    greet(row == row_size - 1, far_sem.at[0], (me, 1))

    arrivals = {}
    for h in range(PARTS):
        for i in range(1, grp_size):
            peer = lax.rem(me + i, grp_size)
            arrivals[h, i] = pltpu.make_async_remote_copy(
                src_ref=slots_v.at[h, :, block_of(peer)],
                dst_ref=recv_v.at[h, i - 1],
                send_sem=send_sem,
                recv_sem=recv_sem.at[h],
                device_id=(peer, row),
                device_id_type=MESH,
            )
    for copy in slot_copies:
        copy.wait()

    def send_to(j, parts, when):
        @pl.when(jnp.logical_and(j < me, when))
        def _():
            i = j + grp_size - me
            for h in parts:
                pltpu.make_async_remote_copy(
                    src_ref=slots_v.at[h, :, pl.ds(j * cap, cap)],
                    dst_ref=recv_v.at[h, i - 1],
                    send_sem=send_sem,
                    recv_sem=recv_sem.at[h],
                    device_id=(j, row),
                    device_id_type=MESH,
                ).start()

    def send_back(allowed, parts, when):
        for j in range(grp_size // 4):
            if allowed(j):
                send_to(j, parts, when(j))
        for some in (parts[: len(parts) // 2], parts[len(parts) // 2 :]):
            for j in range(grp_size // 4, grp_size - 1):
                if some and allowed(j):
                    send_to(j, some, when(j))

    every = list(range(PARTS))
    send_back(lambda j: True, every, lambda j: side >= j % wide)

    far_first = row == row_size - 1
    hop = grp_size // (4 * wide) * wide
    relays = jnp.logical_and(me >= hop, me < 2 * hop)

    def send_one(i, when):
        @pl.when(
            jnp.logical_and(
                jnp.logical_and(when, me + i < grp_size), jnp.logical_not(far_first)
            )
        )
        def _():
            for h in range(PARTS - 1):
                arrivals[h, i].start()

        @pl.when(
            jnp.logical_and(
                jnp.logical_and(when, me + i == grp_size - 1),
                jnp.logical_and(far_first, me >= 2 * hop),
            )
        )
        def _():
            for h in range(PARTS):
                arrivals[h, i].start()

        if i < grp_size - hop:
            @pl.when(
                jnp.logical_and(
                    jnp.logical_and(when, me + i == grp_size - 1),
                    jnp.logical_and(far_first, relays),
                )
            )
            def _():
                for h in range(PARTS):
                    arrivals[h, i].start()
                    held = relay_v.at[h]
                    pltpu.make_async_copy(held, held, relay_recv_sem.at[h]).wait()
                    pltpu.make_async_remote_copy(
                        src_ref=held,
                        dst_ref=recv_v.at[h, i + hop - 1],
                        send_sem=relay_send_sem,
                        recv_sem=recv_sem.at[h],
                        device_id=(grp_size - 1, row),
                        device_id_type=MESH,
                    ).start()

    def hand_over():
        for h in range(PARTS):
            pltpu.make_async_remote_copy(
                src_ref=slots_v.at[h, :, block_of(grp_size - 1)],
                dst_ref=relay_v.at[h],
                send_sem=send_sem,
                recv_sem=relay_recv_sem.at[h],
                device_id=(me + hop, row),
                device_id_type=MESH,
            ).start()

    def send_later(i):
        above = jnp.logical_and(me + i < grp_size, lax.rem(me + i, wide) >= side)

        @pl.when(above)
        def _():
            pl.semaphore_wait(ready_sem.at[me + i], 1)

        if wide == 2 and i % 2 == 0:
            send_one(i - 1, jnp.logical_and(above, side == 1))
        if i == hop:
            pl.when(jnp.logical_and(far_first, me < hop))(hand_over)
        send_one(i, above)
        if i == 1:
            if wide == 2:
                send_back(lambda j: j % wide == 1, every, lambda j: side == 0)

            @pl.when(row == 1)
            def _():
                pl.semaphore_wait(near_sem.at[1], 1)
                pl.semaphore_wait(far_sem.at[0], 1)
                pl.semaphore_signal(
                    far_sem.at[1], inc=1, device_id=(me, row_size - 1), device_id_type=MESH
                )

    def tell_left():
        @pl.when(row == row_size - 1)
        def _():
            pl.semaphore_wait(far_sem.at[1], 1)
            greet(me > 0, near_sem.at[0], (me - 1, row))
            greet(last, near_sem.at[1], right_id)

    def tell_right():
        @pl.when(jnp.logical_and(row == row_size - 1, me < grp_size - 1))
        def _():
            pl.semaphore_wait(near_sem.at[0], 1)
            pl.semaphore_signal(
                near_sem.at[1], inc=1, device_id=right_id, device_id_type=MESH
            )

    def send_rest():
        for i in range(1, grp_size):

            @pl.when(jnp.logical_and(me + i < grp_size - 1, far_first))
            def _():
                for h in range(PARTS - 1):
                    arrivals[h, i].start()

        for i in range(1, grp_size):
            ok = jnp.logical_or(
                me + i < grp_size - 1,
                jnp.logical_and(me + i == grp_size - 1, jnp.logical_not(far_first)),
            )
            pl.when(ok)(arrivals[PARTS - 1, i].start)

    for copy in small_copies:
        copy.wait()

    grp_iota = lax.broadcasted_iota(jnp.int32, (grp_size, elems), 0)
    named = [
        jnp.where(owner_v[c] == grp_iota, np.float32(1), np.float32(0)) for c in range(4)
    ]
    before = (
        lax.broadcasted_iota(jnp.int32, (elems, elems), 0)
        < lax.broadcasted_iota(jnp.int32, (elems, elems), 1)
    )
    running = jnp.dot(
        (named[0] + named[1] + named[2] + named[3]).astype(jnp.bfloat16),
        jnp.where(before, np.float32(1), np.float32(0)).astype(jnp.bfloat16),
        preferred_element_type=jnp.float32,
    )
    targets = []
    for c in range(4):
        rank = jnp.sum(named[c] * running, axis=0, keepdims=True).astype(jnp.int32)
        running = running + named[c]
        slot = me - owner_v[c]
        slot = jnp.where(slot < 0, slot + grp_size, slot)
        targets.append(slot * cap + rank)

    blocks = [jnp.broadcast_to(t // LANES, (2 * part, elems)) for t in targets]
    places = [jnp.broadcast_to(t % LANES, (2 * part, elems)) for t in targets]

    halves = half_weights()
    width = fields * nodes
    lane = lax.broadcasted_iota(jnp.int32, (fields, width), 1)
    spread = jnp.where(
        lane // nodes == lax.broadcasted_iota(jnp.int32, (fields, width), 0),
        np.float32(1),
        np.float32(0),
    )
    mix = jnp.dot(
        mix_v[...], spread, precision=lax.Precision.HIGHEST, preferred_element_type=jnp.float32
    )
    node = lane % nodes
    row_node = lax.broadcasted_iota(jnp.int32, (nodes, elems), 0)
    metric = metric_v[...]
    rows, scales = [], []
    for c in range(4):
        a, b = c % 2, c // 2
        rows.append(mix * pick(node % 4, halves[a]) * pick(node // 4, halves[b]))
        weights = pick(row_node % 4, halves[a]) * pick(row_node // 4, halves[b])
        area = jnp.sum(weights * metric, axis=0, keepdims=True)
        scales.append(jnp.broadcast_to(1.0 / area, (fields, elems)))
    scale = jnp.concatenate(scales, axis=0)
    high, low = split(jnp.concatenate(rows, axis=0))
    matrix = jnp.concatenate(
        [
            jnp.concatenate([high, high], axis=1),
            jnp.concatenate([low, jnp.zeros_like(low)], axis=1),
        ],
        axis=0,
    )
    count = 4 * fields

    def weigh(level):
        x = (gll_v[:, level] * metric[None]).reshape(width, elems)
        return jnp.concatenate(split(x), axis=0)

    send_later(1)
    send_later(2)
    for k in range(chunks):
        gll_copies[k].wait()

        def remap(j, carry):
            level = k * chunk + 2 * j
            data = jnp.concatenate([weigh(level), weigh(level + 1)], axis=1)
            out = jnp.dot(matrix, data, preferred_element_type=jnp.float32)
            out = out[:count] + out[count:]
            mixed_v[level] = out[:, :elems] * scale
            mixed_v[level + 1] = out[:, elems:] * scale
            return carry

        lax.fori_loop(0, chunk // 2, remap, 0, unroll=True)
        if k + 3 < grp_size:
            send_later(k + 3)
        if k == 0:
            tell_left()
    tell_right()

    for i in range(chunks + 3, grp_size):
        send_later(i)
    send_rest()

    quarter = lax.broadcasted_iota(jnp.int32, (fields, elems), 1) // HALO
    hear(jnp.logical_and(odd, row < row_size - 1), near_sem.at[0])
    hear(jnp.logical_or(jnp.logical_and(odd, row != 1), row == 0), near_sem.at[1])
    halo_copies = []
    for h in range(PARTS):
        picked = [None] * 4
        whole = recv_v.at[h]
        pltpu.make_async_copy(whole, whole, recv_sem.at[h]).wait()
        for i in range(grp_size):
            if i == 0:
                held = slots_v[h, :, block_of(me)]
            else:
                held = recv_v[h, i - 1]
            for k in range(cap // LANES):
                source = held[:, k * LANES : (k + 1) * LANES]
                for c in range(4):
                    value = jnp.take_along_axis(
                        source, places[c], axis=1, mode="promise_in_bounds"
                    )
                    if picked[c] is None:
                        picked[c] = value
                    else:
                        block = i * (cap // LANES) + k
                        picked[c] = jnp.where(blocks[c] == block, value, picked[c])
        for c in range(4):
            sel_v[h, c] = picked[c]
        for q in range(packs):
            to_right = to_left = None
            for p in range(pack):
                at = q * pack + p
                level = h * part + at
                mean = None
                for c in range(4):
                    span = pl.ds(c * fields, fields)
                    tend = sel_v[h, c, pl.ds(at, 1)] * jnp.tanh(
                        mixed_v[level, span] + sel_v[h, c, pl.ds(part + at, 1)]
                    )
                    if h == PARTS - 1:
                        tail_ref[at, span] = tend
                    else:
                        tend_v[level, span] = tend
                    mean = tend if mean is None else mean + tend
                mean = mean * np.float32(0.25)
                to_r = pltpu.roll(mean, (HALO * (p + 1)) % elems, 1) if (p + 1) % pack else mean
                to_l = pltpu.roll(mean, HALO * p, 1) if p else mean
                to_right = to_r if p == 0 else jnp.where(quarter == p, to_r, to_right)
                to_left = to_l if p == 0 else jnp.where(quarter == p, to_l, to_left)
            pack_v[0, h * packs + q] = to_right
            pack_v[1, h * packs + q] = to_left
        span = pl.ds(h * packs, packs)
        for way, device in ((0, right_id), (1, left_id)):
            copy = pltpu.make_async_remote_copy(
                src_ref=pack_v.at[way, span],
                dst_ref=halo_v.at[way, span],
                send_sem=halo_send_sem.at[h, way],
                recv_sem=halo_recv_sem.at[h, way],
                device_id=device,
                device_id_type=MESH,
            )
            copy.start()
            halo_copies.append(copy)

    pltpu.make_async_copy(recv_v, recv_v, send_sem).wait()

    @pl.when(jnp.logical_and(far_first, relays))
    def _():
        pltpu.make_async_copy(relay_v, relay_v, relay_send_sem).wait()

    write = nodes_writer(row_size, neighbours_v[...], fields, elems)
    for h in range(PARTS - 1):
        halo_copies[2 * h].wait()
        halo_copies[2 * h + 1].wait()

        def group(q, carry):
            for p in range(pack):
                level = q * pack + p

                def store(f, v, value):
                    done_ref[f, level, pl.ds(8 * v, 8), :] = value

                write(
                    tend_v.at[level], halo_v[0, q], halo_v[1, q], p, work_v.at[p], store
                )
            return carry

        lax.fori_loop(h * packs, (h + 1) * packs, group, 0, unroll=True)
    for copy in halo_copies[2 * PARTS - 2 :]:
        copy.wait()
    for way in range(2):
        for q in range(packs):
            tail_halo_ref[way, q] = halo_v[way, levels // pack - packs + q]


def last_part_kernel(
    row_size, done_ref, tend_ref, halo_ref, neighbours_ref, out_ref, last_v, work_v, sem
):
    fields, part, nodes, elems = last_v.shape
    pack = elems // HALO
    before = done_ref.shape[1]
    copies = []
    for k in range(before // part):
        span = pl.ds(k * part, part)
        copy = pltpu.make_async_copy(done_ref.at[:, span], out_ref.at[:, span], sem.at[k])
        copy.start()
        copies.append(copy)
    write = nodes_writer(row_size, neighbours_ref[...], fields, elems)
    for q in range(part // pack):
        for p in range(pack):
            level = q * pack + p

            def store(f, v, value):
                last_v[f, level, pl.ds(8 * v, 8), :] = value

            write(
                tend_ref.at[level], halo_ref[0, q], halo_ref[1, q], p, work_v.at[level], store
            )
        copy = pltpu.make_async_copy(
            last_v.at[:, pl.ds(q * pack, pack)],
            out_ref.at[:, pl.ds(before + q * pack, pack)],
            sem.at[before // part + q],
        )
        copy.start()
        copies.append(copy)
    for copy in copies:
        copy.wait()


def on_device(gll_state, metric, phys_owner, neighbours, phys_rate, phys_forcing, field_mix):
    fields, levels, nodes, elems = gll_state.shape
    grp_size = lax.axis_size("grp")
    row_size = lax.axis_size("row")
    capacity = phys_rate.shape[1] // grp_size
    cap = -(-capacity // 128) * 128
    if cap != capacity:
        phys_rate, phys_forcing = (
            jnp.pad(
                x.reshape(levels, grp_size, capacity), ((0, 0), (0, 0), (0, cap - capacity))
            ).reshape(levels, grp_size * cap)
            for x in (phys_rate, phys_forcing)
        )
    owner = phys_owner.transpose(1, 2, 0)
    pack = elems // HALO
    part = levels // PARTS
    chunks = 4
    vmem = pl.BlockSpec(memory_space=pltpu.VMEM)
    hbm = pl.BlockSpec(memory_space=pltpu.HBM)
    before = levels - part
    done, tail, tail_halo = pl.pallas_call(
        functools.partial(exchange_kernel, grp_size, row_size),
        out_shape=(
            jax.ShapeDtypeStruct((fields, before, nodes, elems), jnp.float32),
            jax.ShapeDtypeStruct((part, 4 * fields, elems), jnp.float32),
            jax.ShapeDtypeStruct((2, part // pack, fields, elems), jnp.float32),
        ),
        in_specs=[hbm] * 7,
        out_specs=(vmem, vmem, vmem),
        scratch_shapes=[
            pltpu.VMEM((fields, levels, nodes, elems), jnp.float32),
            pltpu.VMEM((nodes, elems), jnp.float32),
            pltpu.VMEM((4, 1, elems), jnp.int32),
            pltpu.VMEM((fields, fields), jnp.float32),
            pltpu.VMEM((4, elems), jnp.int32),
            pltpu.VMEM((PARTS, 2 * part, grp_size * cap), jnp.float32),
            pltpu.VMEM((levels, 4 * fields, elems), jnp.float32),
            pltpu.VMEM((PARTS, grp_size - 1, 2 * part, cap), jnp.float32),
            pltpu.VMEM((PARTS, 4, 2 * part, elems), jnp.float32),
            pltpu.VMEM((before, 4 * fields, elems), jnp.float32),
            pltpu.VMEM((2, levels // pack, fields, elems), jnp.float32),
            pltpu.VMEM((2, levels // pack, fields, elems), jnp.float32),
            pltpu.VMEM((pack, 6, fields, elems), jnp.float32),
            pltpu.SemaphoreType.DMA((chunks,)),
            pltpu.SemaphoreType.DMA((4,)),
            pltpu.SemaphoreType.DMA((PARTS, 2)),
            pltpu.SemaphoreType.DMA,
            pltpu.SemaphoreType.DMA((PARTS,)),
            pltpu.SemaphoreType.DMA((PARTS, 2)),
            pltpu.SemaphoreType.DMA((PARTS, 2)),
            pltpu.SemaphoreType.REGULAR((grp_size,)),
            pltpu.SemaphoreType.REGULAR((2,)),
            pltpu.SemaphoreType.REGULAR((2,)),
            pltpu.VMEM((PARTS, 2 * part, cap), jnp.float32),
            pltpu.SemaphoreType.DMA,
            pltpu.SemaphoreType.DMA((PARTS,)),
        ],
        compiler_params=pltpu.CompilerParams(
            collective_id=0, has_side_effects=True, vmem_limit_bytes=32 * 1024 * 1024
        ),
        name="exchange",
    )(
        *(
            pltpu.with_memory_space_constraint(x, pltpu.HBM)
            for x in (
                gll_state,
                metric,
                owner,
                phys_rate,
                phys_forcing,
                field_mix,
                neighbours,
            )
        )
    )
    anywhere = pl.BlockSpec(memory_space=pl.ANY)
    return pl.pallas_call(
        functools.partial(last_part_kernel, row_size),
        out_shape=jax.ShapeDtypeStruct(gll_state.shape, jnp.float32),
        in_specs=[anywhere, vmem, vmem, vmem],
        out_specs=anywhere,
        scratch_shapes=[
            pltpu.VMEM((fields, part, nodes, elems), jnp.float32),
            pltpu.VMEM((part, 6, fields, elems), jnp.float32),
            pltpu.SemaphoreType.DMA((PARTS - 1 + part // pack,)),
        ],
        compiler_params=pltpu.CompilerParams(vmem_limit_bytes=16 * 1024 * 1024),
        name="last_part",
    )(done, tail, tail_halo, neighbours)


def solution(mesh):
    in_specs = (
        P(None, None, None, ("grp", "row")),
        P(None, ("grp", "row")),
        P(("grp", "row"), None, None),
        P(None, ("grp", "row")),
        P(None, ("grp", "row")),
        P(None, ("grp", "row")),
        P(),
    )
    out_specs = P(None, None, None, ("grp", "row"))
    return jax.shard_map(
        on_device, mesh=mesh, in_specs=in_specs, out_specs=out_specs, check_vma=False
    )
```
